8 devices in a mesh: cp: 8 (over z, y, x, core).
Axes of the slice: x: 2, y: 2, z: 1, core: 2. Of those that a mesh axis runs over, the one named last changes fastest.
Arguments:
- hidden: bfloat16 [8, 2048, 3584], P(None, 'cp')
- grad_out: bfloat16 [8, 2048, 3584], P(None, 'cp')
- positions: int32 [8, 2048], P(None, 'cp')
- seg_ids: int32 [8, 2048], P(None, 'cp')
- w_q: bfloat16 [3584, 3584], replicated
- w_k: bfloat16 [3584, 512], replicated
- w_v: bfloat16 [3584, 512], replicated
- w_o: bfloat16 [3584, 3584], replicated
- norm_gain: bfloat16 [3584], replicated
Outputs:
- output 1: bfloat16 [8, 2048, 3584], P(None, 'cp')
- output 2: bfloat16 [8, 2048, 3584], P(None, 'cp')
- output 3: float32 [3584, 3584], replicated
- output 4: float32 [3584, 512], replicated
- output 5: float32 [3584, 512], replicated
- output 6: float32 [3584, 3584], replicated
- output 7: float32 [3584], replicated
All inputs are finite; a program needn't handle non-finite values.
Results may differ from the reference program's by a relative error of at most 0.0133325.
Values are sent between devices in bfloat16 or wider.
A program may use at most 1 GiB of HBM per device.

```python
import jax
import jax.numpy as jnp
from jax import lax

BATCH = 8
CHUNK = 128
CP_SIZE = 8
D_MODEL = 3584
HEADS = 28
KV_HEADS = 4
HEAD_DIM = 128
NUM_CUTS = 12

SEQ_LEN = 2 * CP_SIZE * CHUNK
GROUP_SIZE = HEADS // KV_HEADS
NORM_EPS = 1e-5
ROPE_BASE = 500000.0
ATTN_SCALE = HEAD_DIM ** -0.5
NEG_BIG = -1e30


def storage_order(glob_rows):
    blocks = glob_rows.reshape(BATCH, 2 * CP_SIZE, CHUNK)
    front_half = blocks[:, :CP_SIZE]
    back_half = blocks[:, CP_SIZE:][:, ::-1]
    return jnp.stack([front_half, back_half], axis=2).reshape(BATCH, SEQ_LEN)


def draw_layout(layout_key):
    key_start, key_len, key_cut = jax.random.split(layout_key, 3)
    long_start = jax.random.randint(key_start, (BATCH, 1), 0, SEQ_LEN // 4 + 1)
    long_end = long_start + SEQ_LEN // 2 + jax.random.randint(key_len, (BATCH, 1), 0, SEQ_LEN // 4 + 1)
    cut_points = jax.random.randint(key_cut, (BATCH, NUM_CUTS), 1, SEQ_LEN)
    keep_cut = (cut_points <= long_start) | (cut_points >= long_end)
    bounds = jnp.concatenate([jnp.where(keep_cut, cut_points, 0), long_start, long_end], axis=1)
    token_idx = jnp.arange(SEQ_LEN)
    passed = (bounds[:, :, None] <= token_idx[None, None, :]) & (bounds[:, :, None] > 0)
    seg_glob = jnp.sum(passed.astype(jnp.int32), axis=1)
    doc_start = jnp.max(jnp.where(passed, bounds[:, :, None], 0), axis=1)
    pos_glob = token_idx[None, :] - doc_start
    return storage_order(pos_glob.astype(jnp.int32)), storage_order(seg_glob.astype(jnp.int32))


def setup_inputs(seed: int = 0) -> dict:
    root_key = jax.random.key(seed)
    key_list = jax.random.split(root_key, 9)
    positions, seg_ids = draw_layout(key_list[0])
    hidden = jax.random.normal(key_list[1], (BATCH, SEQ_LEN, D_MODEL), jnp.float32)
    grad_out = jax.random.normal(key_list[2], (BATCH, SEQ_LEN, D_MODEL), jnp.float32)
    w_q = jax.random.normal(key_list[3], (D_MODEL, HEADS * HEAD_DIM), jnp.float32) * D_MODEL ** -0.5
    w_k = jax.random.normal(key_list[4], (D_MODEL, KV_HEADS * HEAD_DIM), jnp.float32) * D_MODEL ** -0.5
    w_v = jax.random.normal(key_list[5], (D_MODEL, KV_HEADS * HEAD_DIM), jnp.float32) * D_MODEL ** -0.5
    w_o = jax.random.normal(key_list[6], (HEADS * HEAD_DIM, D_MODEL), jnp.float32) * (HEADS * HEAD_DIM) ** -0.5
    norm_gain = jax.random.uniform(key_list[7], (D_MODEL,), jnp.float32, 0.5, 1.5)
    return {
        'hidden': hidden.astype(jnp.bfloat16),
        'grad_out': grad_out.astype(jnp.bfloat16),
        'positions': positions,
        'seg_ids': seg_ids,
        'w_q': w_q.astype(jnp.bfloat16),
        'w_k': w_k.astype(jnp.bfloat16),
        'w_v': w_v.astype(jnp.bfloat16),
        'w_o': w_o.astype(jnp.bfloat16),
        'norm_gain': norm_gain.astype(jnp.bfloat16),
    }


def global_index():
    chunk_slots = jnp.arange(2 * CP_SIZE)
    owner_rank = chunk_slots // 2
    glob_chunk = jnp.where(chunk_slots % 2 == 0, owner_rank, 2 * CP_SIZE - 1 - owner_rank)
    return (glob_chunk[:, None] * CHUNK + jnp.arange(CHUNK)[None, :]).reshape(SEQ_LEN)


def rms_norm(hidden_f32, gain_f32):
    inv_rms = lax.rsqrt(jnp.mean(hidden_f32 * hidden_f32, axis=-1, keepdims=True) + NORM_EPS)
    return (hidden_f32 * inv_rms * gain_f32).astype(jnp.bfloat16)


def rope_tables(positions):
    inv_freq = ROPE_BASE ** (-jnp.arange(0, HEAD_DIM, 2).astype(jnp.float32) / HEAD_DIM)
    angles = positions.astype(jnp.float32)[..., None] * inv_freq
    angles = jnp.concatenate([angles, angles], axis=-1)
    return jnp.cos(angles), jnp.sin(angles)


def rotate(proj_in, cos_t, sin_t):
    half_dim = proj_in.shape[-1] // 2
    turned = jnp.concatenate([-proj_in[..., half_dim:], proj_in[..., :half_dim]], axis=-1)
    return proj_in * cos_t + turned * sin_t


def attention(queries, keys_all, values_all, seg_ids):
    glob_all = global_index()
    n_blocks = 2 * CP_SIZE * KV_HEADS
    q_blocks = queries.reshape(BATCH, 2 * CP_SIZE, CHUNK, KV_HEADS, GROUP_SIZE, HEAD_DIM).transpose(1, 3, 0, 2, 4, 5).reshape(n_blocks, BATCH, CHUNK, GROUP_SIZE, HEAD_DIM)
    glob_blocks = jnp.repeat(glob_all.reshape(2 * CP_SIZE, CHUNK), KV_HEADS, axis=0)
    seg_blocks = jnp.repeat(seg_ids.reshape(BATCH, 2 * CP_SIZE, CHUNK).transpose(1, 0, 2), KV_HEADS, axis=0)
    head_ids = jnp.tile(jnp.arange(KV_HEADS), 2 * CP_SIZE)
    keys_t = jnp.moveaxis(keys_all, 2, 0)
    values_t = jnp.moveaxis(values_all, 2, 0)

    def block_attend(operands):
        q_blk, glob_q, seg_q, head_id = operands
        scores = jnp.einsum('bqgd,bsd->bgqs', q_blk, keys_t[head_id]) * ATTN_SCALE
        allowed = (seg_q[:, :, None] == seg_ids[:, None, :]) & (glob_q[:, None] >= glob_all[None, :])[None]
        attn_probs = jax.nn.softmax(jnp.where(allowed[:, None], scores, NEG_BIG), axis=-1)
        attn_probs = attn_probs.astype(jnp.bfloat16).astype(jnp.float32)
        return jnp.einsum('bgqs,bsd->bqgd', attn_probs, values_t[head_id])

    out_blocks = lax.map(jax.checkpoint(block_attend), (q_blocks, glob_blocks, seg_blocks, head_ids))
    attn_out = out_blocks.reshape(2 * CP_SIZE, KV_HEADS, BATCH, CHUNK, GROUP_SIZE, HEAD_DIM).transpose(2, 0, 3, 1, 4, 5)
    return attn_out.reshape(BATCH * SEQ_LEN, HEADS * HEAD_DIM).astype(jnp.bfloat16).astype(jnp.float32)


def forward(hidden, positions, seg_ids, wq_f32, wk_f32, wv_f32, wo_f32, gain_f32):
    hidden_f32 = hidden.astype(jnp.float32)
    normed = rms_norm(hidden_f32, gain_f32).astype(jnp.float32).reshape(BATCH * SEQ_LEN, D_MODEL)
    cos_t, sin_t = rope_tables(positions)
    q_lin = jnp.dot(normed, wq_f32, preferred_element_type=jnp.float32).reshape(BATCH, SEQ_LEN, KV_HEADS, GROUP_SIZE, HEAD_DIM)
    queries = rotate(q_lin, cos_t[:, :, None, None], sin_t[:, :, None, None]).astype(jnp.bfloat16).astype(jnp.float32)
    k_lin = jnp.dot(normed, wk_f32, preferred_element_type=jnp.float32).reshape(BATCH, SEQ_LEN, KV_HEADS, HEAD_DIM)
    keys_all = rotate(k_lin, cos_t[:, :, None], sin_t[:, :, None]).astype(jnp.bfloat16).astype(jnp.float32)
    values_all = jnp.dot(normed, wv_f32, preferred_element_type=jnp.float32).astype(jnp.bfloat16).astype(jnp.float32).reshape(BATCH, SEQ_LEN, KV_HEADS, HEAD_DIM)
    attn_flat = attention(queries, keys_all, values_all, seg_ids)
    proj_out = jnp.dot(attn_flat, wo_f32, preferred_element_type=jnp.float32).reshape(BATCH, SEQ_LEN, D_MODEL)
    return (hidden_f32 + proj_out).astype(jnp.bfloat16)


def reference(hidden, grad_out, positions, seg_ids, w_q, w_k, w_v, w_o, norm_gain):
    def run_block(hidden_in, wq_f32, wk_f32, wv_f32, wo_f32, gain_f32):
        return forward(hidden_in, positions, seg_ids, wq_f32, wk_f32, wv_f32, wo_f32, gain_f32)

    block_out, pullback = jax.vjp(run_block, hidden, w_q.astype(jnp.float32), w_k.astype(jnp.float32), w_v.astype(jnp.float32), w_o.astype(jnp.float32), norm_gain.astype(jnp.float32))
    grad_hidden, grad_wq, grad_wk, grad_wv, grad_wo, grad_gain = pullback(grad_out)
    return block_out, grad_hidden, grad_wq, grad_wk, grad_wv, grad_wo, grad_gain
```

```python
import functools
import math

import jax
import jax.numpy as jnp
from jax import lax
from jax.experimental import pallas as pl
from jax.experimental.pallas import tpu as pltpu
from jax.sharding import PartitionSpec as P


HEAD_DIM = 128
NORM_EPS = 1e-5
ROPE_BASE = 500000.0
NEG_BIG = -1e30
SCALE = HEAD_DIM ** -0.5
LOG2E = math.log2(math.e)
SCALE2 = SCALE * LOG2E
BF16 = jnp.bfloat16
F32 = jnp.float32
VMEM_LIMIT = 60 * 1024 * 1024
NT = (((1,), (1,)), ((), ()))
NN = (((1,), (0,)), ((), ()))
TN = (((0,), (0,)), ((), ()))


def dotf(a, b, dims):
    return lax.dot_general(a, b, dims, preferred_element_type=F32)


def rows8(x):
    return x.reshape(x.shape[0] // 8, 8, x.shape[1]) if x.ndim == 2 else x.reshape(x.shape[0] * 8, x.shape[2])


def all8(x):
    return jnp.broadcast_to(x, (8, x.shape[1]))


def params(**kw):
    return pltpu.CompilerParams(vmem_limit_bytes=VMEM_LIMIT, **kw)


def norm_kv_kernel(x_ref, g_ref, wk_ref, wv_ref, cos_ref, sin_ref, n_ref, *kv_refs):
    n_tok = x_ref.shape[1]
    half = n_tok // 2
    x = x_ref[0].astype(F32)
    inv = lax.rsqrt(jnp.mean(x * x, axis=-1, keepdims=True) + NORM_EPS)
    normed = rows8(rows8(x * inv) * g_ref[...]).astype(BF16)
    n_ref[...] = normed
    k_all = dotf(normed, wk_ref[...], NN)
    v_all = dotf(normed, wv_ref[...], NN)
    cos_t, sin_t = cos_ref[0], sin_ref[0]
    for h, kv_ref in enumerate(kv_refs):
        cols = slice(h * HEAD_DIM, (h + 1) * HEAD_DIM)
        k = k_all[:, cols]
        k = (k * cos_t + pltpu.roll(k, HEAD_DIM // 2, 1) * sin_t).astype(BF16)
        v = v_all[:, cols].astype(BF16)
        kv_ref[0, 0, :, :HEAD_DIM] = k[:half]
        kv_ref[1, 0, :, :HEAD_DIM] = k[half:]
        kv_ref[0, 0, :, HEAD_DIM:] = v[:half]
        kv_ref[1, 0, :, HEAD_DIM:] = v[half:]


def norm_kv(hidden, gain, w_k, w_v, cos_t, sin_t):
    n_batch, n_tok, d_model = hidden.shape
    kv_heads = w_k.shape[1] // HEAD_DIM
    half = n_tok // 2
    row = pl.BlockSpec((1, n_tok, HEAD_DIM), lambda i: (i, 0, 0))
    whole = pl.BlockSpec(w_k.shape, lambda i: (0, 0))
    out = pl.pallas_call(
        norm_kv_kernel,
        grid=(n_batch,),
        in_specs=[
            pl.BlockSpec((1, n_tok, d_model), lambda i: (i, 0, 0)),
            pl.BlockSpec((8, d_model), lambda i: (0, 0)),
            whole, whole, row, row,
        ],
        out_specs=[pl.BlockSpec((n_tok, d_model), lambda i: (i, 0))]
        + [pl.BlockSpec((2, 1, half, 2 * HEAD_DIM), lambda i: (0, i, 0, 0))] * kv_heads,
        out_shape=[jax.ShapeDtypeStruct((n_batch * n_tok, d_model), BF16)]
        + [jax.ShapeDtypeStruct((2, n_batch, half, 2 * HEAD_DIM), BF16)] * kv_heads,
        compiler_params=params(),
        cost_estimate=pl.CostEstimate(flops=4 * n_batch * n_tok * d_model * w_k.shape[1], bytes_accessed=4 * hidden.size + 4 * w_k.size, transcendentals=0),
        name="norm_kv",
    )(hidden, jnp.broadcast_to(gain.astype(F32), (8, d_model)), w_k, w_v, cos_t, sin_t)
    return out[0], out[1:]


def q_proj_kernel(n_ref, w_ref, cos_ref, sin_ref, q_ref):
    q = dotf(n_ref[...], w_ref[...], NN)
    cos_t, sin_t = cos_ref[...], sin_ref[...]
    for g in range(q.shape[1] // HEAD_DIM):
        cols = slice(g * HEAD_DIM, (g + 1) * HEAD_DIM)
        qg = q[:, cols]
        q_ref[:, cols] = (qg * cos_t + pltpu.roll(qg, HEAD_DIM // 2, 1) * sin_t).astype(BF16)


def q_proj(normed, w_q, cos_t, sin_t, h, width, tile=512):
    n_all, d_model = normed.shape
    return pl.pallas_call(
        q_proj_kernel,
        grid=(n_all // tile,),
        in_specs=[
            pl.BlockSpec((tile, d_model), lambda i: (i, 0)),
            pl.BlockSpec((d_model, width), lambda i: (0, h)),
            pl.BlockSpec((tile, HEAD_DIM), lambda i: (i, 0)),
            pl.BlockSpec((tile, HEAD_DIM), lambda i: (i, 0)),
        ],
        out_specs=pl.BlockSpec((tile, width), lambda i: (i, 0)),
        out_shape=jax.ShapeDtypeStruct((n_all, width), BF16),
        compiler_params=params(),
        cost_estimate=pl.CostEstimate(flops=2 * n_all * d_model * width, bytes_accessed=2 * n_all * d_model + 2 * d_model * width, transcendentals=0),
    )(normed, w_q, cos_t.reshape(n_all, HEAD_DIM), sin_t.reshape(n_all, HEAD_DIM))


def pair_list(group):
    return [(2 * j, min(2, group - 2 * j)) for j in range((group + 1) // 2)]


def block_place(b, n_dev):
    half = (b >= n_dev // 2).astype(jnp.int32)
    dev = 2 * jnp.where(half == 1, n_dev - 1 - b, b)
    return dev, half


def block_mask(b, half, lo_row, hi_row):
    key = rows8(lax.broadcasted_iota(jnp.int32, (2 * HEAD_DIM, HEAD_DIM), 0))
    key = (key ^ (half * HEAD_DIM)) + b * (2 * HEAD_DIM)
    return (key >= lo_row) & (key <= hi_row)


def for_blocks(c, row, lo_sm, full_sm, qc_sm, step):
    lo, full, last = lo_sm[row, c], full_sm[row, c], qc_sm[c] // 2

    def masked(t, carry):
        step(jnp.where(lo + t < full, lo + t, last), True)
        return carry

    def plain(b, carry):
        step(b, False)
        return carry

    lax.fori_loop(0, full - lo + 1, masked, 0)
    lax.fori_loop(full, last, plain, 0)


def attn_fwd_kernel(lo_sm, full_sm, qc_sm, q_ref, kv_ref, lim_ref, o_ref, lse_ref, vt, qs, m_ref, l_ref, acc, *, group):
    row = pl.program_id(0)
    n_dev = kv_ref.shape[0]
    chunk = HEAD_DIM

    def key_block(b):
        dev, half = block_place(b, n_dev)
        return kv_ref.at[pl.ds(dev, 2), half, 0]

    def turn(b, carry):
        v = key_block(b)[:, :, HEAD_DIM:].reshape(2 * chunk, HEAD_DIM)
        vt[b] = v.T
        return carry

    lax.fori_loop(jnp.minimum(lo_sm[row, 0], lo_sm[row, 1]), qc_sm[1] // 2 + 1, turn, 0)

    def one_chunk(c, carry):
        base = pl.multiple_of(c * chunk, chunk)
        for g in range(group):
            qs[g * chunk:(g + 1) * chunk, :] = q_ref[pl.ds(base, chunk), g * HEAD_DIM:(g + 1) * HEAD_DIM]
        m_ref[...] = jnp.full_like(m_ref, NEG_BIG)
        l_ref[...] = jnp.zeros_like(l_ref)
        acc[...] = jnp.zeros_like(acc)
        lo_row, hi_row = lim_ref[0, c, 0], lim_ref[0, c, 1]

        def step(b, use_mask):
            _, half = block_place(b, n_dev)
            k = key_block(b)[:, :, :HEAD_DIM].reshape(2 * chunk, HEAD_DIM)
            v_t = vt[b]
            if use_mask:
                ok = block_mask(b, half, lo_row, hi_row)
            spans = [(slice(g0 * chunk, (g0 + ng) * chunk), ng) for g0, ng in pair_list(group)]
            ahead = dotf(k, qs[spans[0][0], :], NT)
            for j, (cols, ng) in enumerate(spans):
                s = rows8(ahead)
                if j + 1 < len(spans):
                    ahead = dotf(k, qs[spans[j + 1][0], :], NT)
                if use_mask:
                    s = jnp.concatenate([jnp.where(ok, s[:, :, i * chunk:(i + 1) * chunk], NEG_BIG) for i in range(ng)], axis=2)
                m_old = m_ref[:, cols]
                m_new = jnp.maximum(m_old, all8(jnp.max(jnp.max(s, axis=0), axis=0, keepdims=True)))
                p = jnp.exp2((s - m_new) * SCALE2)
                alpha = jnp.exp2((m_old - m_new) * SCALE2)
                m_ref[:, cols] = m_new
                l_ref[:, cols] = l_ref[:, cols] * alpha + jnp.sum(p, axis=0)
                acc[:, cols] = rows8(rows8(acc[:, cols]) * alpha) + dotf(v_t, rows8(p).astype(BF16), NN)

        for_blocks(c, row, lo_sm, full_sm, qc_sm, step)
        l_all = all8(jnp.sum(l_ref[...], axis=0, keepdims=True))
        inv_l = 1.0 / l_all
        lse_ref[0, c] = m_ref[...] * SCALE2 + jnp.log(l_all) * LOG2E
        for g in range(group):
            cols = slice(g * chunk, (g + 1) * chunk)
            o_t = rows8(rows8(acc[:, cols]) * inv_l[:, cols])
            o_ref[pl.ds(base, chunk), cols] = o_t.T.astype(BF16)
        return carry

    lax.fori_loop(0, 2, one_chunk, 0)


def attn_cost(n_rows, n_dev, width, n_mat):
    pairs = n_rows * (2 * n_dev + 1) * 128 * 128 * (width // HEAD_DIM)
    return pl.CostEstimate(flops=4 * n_mat * pairs * HEAD_DIM, bytes_accessed=8 * n_rows * 256 * width, transcendentals=pairs)


def attn_fwd(scalars, q, kv, limits):
    n_all, width = q.shape
    n_dev, _, n_rows, chunk, _ = kv.shape
    group = width // HEAD_DIM
    n_tok = n_all // n_rows
    return pl.pallas_call(
        functools.partial(attn_fwd_kernel, group=group),
        grid_spec=pltpu.PrefetchScalarGridSpec(
            num_scalar_prefetch=3,
            grid=(n_rows,),
            in_specs=[
                pl.BlockSpec((n_tok, width), lambda i, *_: (i, 0)),
                pl.BlockSpec((n_dev, 2, 1, chunk, 2 * HEAD_DIM), lambda i, *_: (0, 0, i, 0, 0)),
                pl.BlockSpec((1, 2, 2, 8, chunk), lambda i, *_: (i, 0, 0, 0, 0)),
            ],
            out_specs=[
                pl.BlockSpec((n_tok, width), lambda i, *_: (i, 0)),
                pl.BlockSpec((1, 2, 8, width), lambda i, *_: (i, 0, 0, 0)),
            ],
            scratch_shapes=[
                pltpu.VMEM((n_dev, HEAD_DIM, 2 * chunk), BF16),
                pltpu.VMEM((group * chunk, HEAD_DIM), BF16),
                pltpu.VMEM((8, width), F32),
                pltpu.VMEM((8, width), F32),
                pltpu.VMEM((HEAD_DIM, width), F32),
            ],
        ),
        out_shape=[
            jax.ShapeDtypeStruct((n_all, width), BF16),
            jax.ShapeDtypeStruct((n_rows, 2, 8, width), F32),
        ],
        compiler_params=params(),
        cost_estimate=attn_cost(n_rows, n_dev, width, 2),
    )(*scalars, q, kv, limits)


def attn_bwd_kernel(lo_sm, full_sm, qc_sm, q_ref, kv_ref, lim_ref, do_ref, lse_ref, dl_ref, cos_ref, sin_ref, dq_ref, dkv_ref, kt, qs, dos, dqt, *, group):
    row = pl.program_id(0)
    n_dev = kv_ref.shape[0]
    chunk = HEAD_DIM
    dkv_ref[...] = jnp.zeros_like(dkv_ref)

    def key_block(b):
        dev, half = block_place(b, n_dev)
        return kv_ref.at[pl.ds(dev, 2), half, 0]

    def turn(b, carry):
        k = key_block(b)[:, :, :HEAD_DIM].reshape(2 * chunk, HEAD_DIM)
        kt[b] = k.T
        return carry

    lax.fori_loop(jnp.minimum(lo_sm[row, 0], lo_sm[row, 1]), qc_sm[1] // 2 + 1, turn, 0)

    def one_chunk(c, carry):
        base = pl.multiple_of(c * chunk, chunk)
        for g in range(group):
            cols = slice(g * HEAD_DIM, (g + 1) * HEAD_DIM)
            qs[g * chunk:(g + 1) * chunk, :] = q_ref[pl.ds(base, chunk), cols]
            dos[g * chunk:(g + 1) * chunk, :] = do_ref[pl.ds(base, chunk), cols]
        dqt[...] = jnp.zeros_like(dqt)
        lo_row, hi_row = lim_ref[0, c, 0], lim_ref[0, c, 1]

        def step(b, use_mask):
            dev, half = block_place(b, n_dev)
            kv = key_block(b)[...].reshape(2 * chunk, 2 * HEAD_DIM)
            k, v = kv[:, :HEAD_DIM], kv[:, HEAD_DIM:]
            k_t = kt[b]
            if use_mask:
                ok = block_mask(b, half, lo_row, hi_row)
            dk = jnp.zeros((2 * chunk, HEAD_DIM), F32)
            dv = jnp.zeros((2 * chunk, HEAD_DIM), F32)
            spans = [(slice(g0 * chunk, (g0 + ng) * chunk), ng) for g0, ng in pair_list(group)]

            def scores(j):
                cols = spans[j][0]
                return dotf(k, qs[cols, :], NT), dotf(v, dos[cols, :], NT)

            ahead = scores(0)
            for j, (cols, ng) in enumerate(spans):
                s, dp = ahead
                if j + 1 < len(spans):
                    ahead = scores(j + 1)
                p = jnp.exp2(rows8(s) * SCALE2 - lse_ref[0, c, :, cols])
                if use_mask:
                    p = jnp.concatenate([jnp.where(ok, p[:, :, i * chunk:(i + 1) * chunk], 0.0) for i in range(ng)], axis=2)
                ds = rows8(p * (rows8(dp) - dl_ref[0, c, :, cols])).astype(BF16)
                dv = dv + dotf(rows8(p).astype(BF16), dos[cols, :], NN)
                dk = dk + dotf(ds, qs[cols, :], NN)
                dqt[:, cols] += dotf(k_t, ds, NN)
            out = dkv_ref.at[pl.ds(dev, 2), half, 0]
            out[:, :, :HEAD_DIM] += (dk * SCALE).reshape(2, chunk, HEAD_DIM)
            out[:, :, HEAD_DIM:] += dv.reshape(2, chunk, HEAD_DIM)

        for_blocks(c, row, lo_sm, full_sm, qc_sm, step)
        cos_t, sin_t = cos_ref[0, c], sin_ref[0, c]
        for g in range(group):
            cols = slice(g * chunk, (g + 1) * chunk)
            d = dqt[:, cols] * SCALE
            a, b = d[:HEAD_DIM // 2], d[HEAD_DIM // 2:]
            turned = jnp.concatenate([a * cos_t + b * sin_t, b * cos_t - a * sin_t], axis=0)
            dq_ref[pl.ds(base, chunk), cols] = turned.T.astype(BF16)
        return carry

    lax.fori_loop(0, 2, one_chunk, 0)


def attn_bwd(scalars, q, kv, limits, d_o, lse, delta, cos_c, sin_c):
    n_all, width = q.shape
    n_dev, _, n_rows, chunk, _ = kv.shape
    group = width // HEAD_DIM
    n_tok = n_all // n_rows
    tok = pl.BlockSpec((n_tok, width), lambda i, *_: (i, 0))
    kvs = pl.BlockSpec((n_dev, 2, 1, chunk, 2 * HEAD_DIM), lambda i, *_: (0, 0, i, 0, 0))
    stat = pl.BlockSpec((1, 2, 8, width), lambda i, *_: (i, 0, 0, 0))
    rope = pl.BlockSpec((1, 2, HEAD_DIM // 2, chunk), lambda i, *_: (i, 0, 0, 0))
    return pl.pallas_call(
        functools.partial(attn_bwd_kernel, group=group),
        grid_spec=pltpu.PrefetchScalarGridSpec(
            num_scalar_prefetch=3,
            grid=(n_rows,),
            in_specs=[tok, kvs, pl.BlockSpec((1, 2, 2, 8, chunk), lambda i, *_: (i, 0, 0, 0, 0)), tok, stat, stat, rope, rope],
            out_specs=[tok, kvs],
            scratch_shapes=[
                pltpu.VMEM((n_dev, HEAD_DIM, 2 * chunk), BF16),
                pltpu.VMEM((group * chunk, HEAD_DIM), BF16),
                pltpu.VMEM((group * chunk, HEAD_DIM), BF16),
                pltpu.VMEM((HEAD_DIM, width), F32),
            ],
        ),
        out_shape=[
            jax.ShapeDtypeStruct((n_all, width), BF16),
            jax.ShapeDtypeStruct(kv.shape, F32),
        ],
        compiler_params=params(),
        cost_estimate=attn_cost(n_rows, n_dev, width, 5),
    )(*scalars, q, kv, limits, d_o, lse, delta, cos_c, sin_c)


def copy_kernel(i_ref, o_ref):
    o_ref[...] = i_ref[...]


def copy_out(x, tile=448):
    spec = pl.BlockSpec((tile, x.shape[1]), lambda i: (i, 0))
    return pl.pallas_call(
        copy_kernel,
        grid=(x.shape[0] // tile,),
        in_specs=[spec],
        out_specs=spec,
        out_shape=jax.ShapeDtypeStruct(x.shape, x.dtype),
        compiler_params=params(),
        cost_estimate=pl.CostEstimate(flops=x.size, bytes_accessed=8 * x.size, transcendentals=0),
        name="copy_out",
    )(x)


def solution(mesh):
    n_dev = mesh.shape['cp']

    def block(hidden, grad_out, positions, seg_ids, w_q, w_k, w_v, w_o, norm_gain):
        n_batch, n_tok, d_model = hidden.shape
        n_all = n_batch * n_tok
        chunk = n_tok // 2
        kv_heads = w_k.shape[1] // HEAD_DIM
        width = w_q.shape[1] // kv_heads
        group = width // HEAD_DIM
        heads = range(kv_heads)
        rank = lax.axis_index('cp')

        q_chunks = jnp.stack([rank, 2 * n_dev - 1 - rank]).astype(jnp.int32)
        glob = (q_chunks[:, None] * chunk + jnp.arange(chunk, dtype=jnp.int32)[None, :])
        pos_c = positions.reshape(n_batch, 2, chunk)
        doc_start = glob[None] - pos_c
        limits = jnp.stack([doc_start, jnp.broadcast_to(glob[None], doc_start.shape)], axis=2)
        limits = jnp.broadcast_to(limits[:, :, :, None], (n_batch, 2, 2, 8, chunk))
        blk = 2 * chunk
        last = q_chunks // 2
        lo_blk = doc_start[:, :, 0] // blk
        full_blk = jnp.minimum((doc_start[:, :, -1] + blk - 1) // blk, last[None, :])
        scalars = (lo_blk, full_blk, q_chunks)

        inv_freq = ROPE_BASE ** (-jnp.arange(0, HEAD_DIM, 2).astype(F32) / HEAD_DIM)
        pos_f = positions.astype(F32)
        ang = pos_f[..., None] * inv_freq
        cos_h, sin_h = jnp.cos(ang), jnp.sin(ang)
        cos_t = jnp.concatenate([cos_h, cos_h], axis=-1)
        sin_t = jnp.concatenate([-sin_h, sin_h], axis=-1)
        cos_c = jnp.swapaxes(cos_h.reshape(n_batch, 2, chunk, HEAD_DIM // 2), 2, 3)
        sin_c = jnp.swapaxes(sin_h.reshape(n_batch, 2, chunk, HEAD_DIM // 2), 2, 3)

        cos_c, sin_c, cos_t, sin_t = lax.optimization_barrier((cos_c, sin_c, cos_t, sin_t))
        normed, kv_loc = norm_kv(hidden, norm_gain, w_k, w_v, cos_t, sin_t)
        kv_all = []
        for h in heads:
            kv_all.append(lax.all_gather(kv_loc[h], 'cp', axis=0, tiled=False))

        dy = grad_out.reshape(n_all, d_model)
        scatter = functools.partial(lax.psum_scatter, axis_name='cp', scatter_dimension=0, tiled=True)
        gather = functools.partial(lax.all_gather, axis_name='cp', tiled=True)
        q, attn, lse, gwo = [], [], [], []
        for h in heads:
            q.append(q_proj(normed, w_q, cos_t, sin_t, h, width))
            o_h, lse_h = attn_fwd(scalars, q[h], kv_all[h], limits)
            attn.append(o_h)
            lse.append(lse_h)
            part = dotf(o_h, dy, TN)
            gwo.append(scatter(part))

        dq, dkv, gwq = [], [], []
        for h in heads:
            d_attn = dotf(dy, w_o[h * width:(h + 1) * width], NT).astype(BF16)
            delta = jnp.sum((attn[h].astype(F32) * d_attn.astype(F32)).reshape(n_batch, 2, chunk, group, HEAD_DIM), axis=-1)
            delta = jnp.broadcast_to(jnp.swapaxes(delta, 2, 3).reshape(n_batch, 2, 1, width), (n_batch, 2, 8, width))
            dq_h, dkv_h = attn_bwd(scalars, q[h], kv_all[h], limits, d_attn, lse[h], delta, cos_c, sin_c)
            dq.append(dq_h)
            dkv.append(lax.psum_scatter(dkv_h, 'cp', scatter_dimension=0, tiled=False))
            part = dotf(normed, dq_h, TN)
            gwq.append(scatter(part))
        gwo_all = gather(jnp.stack(gwo), axis=1).reshape(w_o.shape)

        attn_flat = jnp.concatenate(attn, axis=1)
        proj_out = dotf(attn_flat, w_o, NN).reshape(hidden.shape)
        block_out = (hidden.astype(F32) + proj_out).astype(BF16)
        dq_flat = jnp.concatenate(dq, axis=1)
        d_norm_q = dotf(dq_flat, w_q, NT)
        gwo_all, d_norm_q, block_out = lax.optimization_barrier((gwo_all, d_norm_q, block_out))
        grad_wo = copy_out(gwo_all)
        grad_wo, own_last = lax.optimization_barrier((grad_wo, dkv[-1]))
        dkv[-1] = own_last

        dk_lin, dv_lin = [], []
        cos_k, sin_k = cos_t.reshape(n_batch, 2, chunk, HEAD_DIM), sin_t.reshape(n_batch, 2, chunk, HEAD_DIM)
        for h in heads:
            own = jnp.swapaxes(dkv[h], 0, 1)
            dk, dv = own[..., :HEAD_DIM], own[..., HEAD_DIM:]
            swapped = jnp.concatenate([dk[..., HEAD_DIM // 2:], dk[..., :HEAD_DIM // 2]], axis=-1)
            dk_lin.append((dk * cos_k - swapped * sin_k).astype(BF16).reshape(n_all, HEAD_DIM))
            dv_lin.append(dv.astype(BF16).reshape(n_all, HEAD_DIM))
        dk_flat = jnp.concatenate(dk_lin, axis=1)
        dv_flat = jnp.concatenate(dv_lin, axis=1)
        part_k, part_v = dotf(normed, dk_flat, TN), dotf(normed, dv_flat, TN)
        gwk = scatter(part_k)
        gwv = scatter(part_v)
        gwq_own, dk_flat, dv_flat = lax.optimization_barrier((jnp.concatenate(gwq, axis=1), dk_flat, dv_flat))
        gwq_all = gather(gwq_own, axis=0)

        d_norm_kv = dotf(dk_flat, w_k, NT) + dotf(dv_flat, w_v, NT)
        d_normed = (d_norm_q + d_norm_kv).astype(BF16).astype(F32)
        x = hidden.astype(F32).reshape(n_all, d_model)
        inv = lax.rsqrt(jnp.mean(x * x, axis=-1, keepdims=True) + NORM_EPS)
        xn = x * inv
        u = d_normed * norm_gain.astype(F32)
        d_x = inv * (u - xn * jnp.mean(u * xn, axis=-1, keepdims=True))
        grad_hidden = (dy.astype(F32) + d_x).astype(BF16).reshape(hidden.shape)
        grad_gain = lax.psum(jnp.sum(d_normed * xn, axis=0), 'cp')
        gwk_all = gather(gwk, axis=0)
        gwv_all = gather(gwv, axis=0)
        gwq_all, grad_hidden, grad_gain = lax.optimization_barrier((gwq_all, grad_hidden, grad_gain))
        grad_wq = copy_out(gwq_all)
        grad_wk, grad_wv = copy_out(gwk_all), copy_out(gwv_all)
        return block_out, grad_hidden, grad_wq, grad_wk, grad_wv, grad_wo, grad_gain

    seq_spec = P(None, 'cp', None)
    tok_spec = P(None, 'cp')
    full = P()
    return jax.shard_map(block, mesh=mesh, in_specs=(seq_spec, seq_spec, tok_spec, tok_spec, full, full, full, full, full), out_specs=(seq_spec, seq_spec, full, full, full, full, full), check_vma=False)
```

```python
import functools
import math

import jax
import jax.numpy as jnp
from jax import lax
from jax.experimental import pallas as pl
from jax.experimental.pallas import tpu as pltpu
from jax.sharding import PartitionSpec as P


HEAD_DIM = 128
NORM_EPS = 1e-5
ROPE_BASE = 500000.0
NEG_BIG = -1e30
SCALE = HEAD_DIM ** -0.5
LOG2E = math.log2(math.e)
SCALE2 = SCALE * LOG2E
BF16 = jnp.bfloat16
F32 = jnp.float32
VMEM_LIMIT = 60 * 1024 * 1024
NT = (((1,), (1,)), ((), ()))
NN = (((1,), (0,)), ((), ()))
TN = (((0,), (0,)), ((), ()))


def dotf(a, b, dims):
    return lax.dot_general(a, b, dims, preferred_element_type=F32)


def rows8(x):
    return x.reshape(x.shape[0] // 8, 8, x.shape[1]) if x.ndim == 2 else x.reshape(x.shape[0] * 8, x.shape[2])


def all8(x):
    return jnp.broadcast_to(x, (8, x.shape[1]))


def params(**kw):
    return pltpu.CompilerParams(vmem_limit_bytes=VMEM_LIMIT, **kw)


def norm_kv_kernel(x_ref, g_ref, wk_ref, wv_ref, cos_ref, sin_ref, n_ref, *kv_refs):
    n_tok = x_ref.shape[1]
    half = n_tok // 2
    x = x_ref[0].astype(F32)
    inv = lax.rsqrt(jnp.mean(x * x, axis=-1, keepdims=True) + NORM_EPS)
    normed = rows8(rows8(x * inv) * g_ref[...]).astype(BF16)
    n_ref[...] = normed
    k_all = dotf(normed, wk_ref[...], NN)
    v_all = dotf(normed, wv_ref[...], NN)
    cos_t, sin_t = cos_ref[0], sin_ref[0]
    for h in range(wk_ref.shape[1] // HEAD_DIM):
        kv_ref, at = (kv_refs[0], 0) if h == 0 else (kv_refs[1], h - 1)
        cols = slice(h * HEAD_DIM, (h + 1) * HEAD_DIM)
        k = k_all[:, cols]
        k = (k * cos_t + pltpu.roll(k, HEAD_DIM // 2, 1) * sin_t).astype(BF16)
        v = v_all[:, cols].astype(BF16)
        for i in range(2):
            kv_ref[at, i, 0, :, :HEAD_DIM] = k[i * half:(i + 1) * half]
            kv_ref[at, i, 0, :, HEAD_DIM:] = v[i * half:(i + 1) * half]


def norm_kv(hidden, gain, w_k, w_v, cos_t, sin_t):
    n_batch, n_tok, d_model = hidden.shape
    kv_heads = w_k.shape[1] // HEAD_DIM
    half = n_tok // 2
    row = pl.BlockSpec((1, n_tok, HEAD_DIM), lambda i: (i, 0, 0))
    whole = pl.BlockSpec(w_k.shape, lambda i: (0, 0))
    parts = [1, kv_heads - 1] if kv_heads > 1 else [1]
    return pl.pallas_call(
        norm_kv_kernel,
        grid=(n_batch,),
        in_specs=[
            pl.BlockSpec((1, n_tok, d_model), lambda i: (i, 0, 0)),
            pl.BlockSpec((8, d_model), lambda i: (0, 0)),
            whole, whole, row, row,
        ],
        out_specs=[pl.BlockSpec((n_tok, d_model), lambda i: (i, 0))]
        + [pl.BlockSpec((n, 2, 1, half, 2 * HEAD_DIM), lambda i: (0, 0, i, 0, 0)) for n in parts],
        out_shape=[jax.ShapeDtypeStruct((n_batch * n_tok, d_model), BF16)]
        + [jax.ShapeDtypeStruct((n, 2, n_batch, half, 2 * HEAD_DIM), BF16) for n in parts],
        compiler_params=params(),
        cost_estimate=pl.CostEstimate(flops=4 * n_batch * n_tok * d_model * w_k.shape[1], bytes_accessed=4 * hidden.size + 4 * w_k.size, transcendentals=0),
        name="norm_kv",
    )(hidden, jnp.broadcast_to(gain.astype(F32), (8, d_model)), w_k, w_v, cos_t, sin_t)


def q_proj_kernel(n_ref, w_ref, cos_ref, sin_ref, q_ref):
    q = dotf(n_ref[...], w_ref[...], NN)
    cos_t, sin_t = cos_ref[...], sin_ref[...]
    for g in range(q.shape[1] // HEAD_DIM):
        cols = slice(g * HEAD_DIM, (g + 1) * HEAD_DIM)
        qg = q[:, cols]
        q_ref[:, cols] = (qg * cos_t + pltpu.roll(qg, HEAD_DIM // 2, 1) * sin_t).astype(BF16)


def q_proj(normed, w_q, cos_t, sin_t, h, width, tile=512):
    n_all, d_model = normed.shape
    return pl.pallas_call(
        q_proj_kernel,
        grid=(n_all // tile,),
        in_specs=[
            pl.BlockSpec((tile, d_model), lambda i: (i, 0)),
            pl.BlockSpec((d_model, width), lambda i: (0, h)),
            pl.BlockSpec((tile, HEAD_DIM), lambda i: (i, 0)),
            pl.BlockSpec((tile, HEAD_DIM), lambda i: (i, 0)),
        ],
        out_specs=pl.BlockSpec((tile, width), lambda i: (i, 0)),
        out_shape=jax.ShapeDtypeStruct((n_all, width), BF16),
        compiler_params=params(),
        cost_estimate=pl.CostEstimate(flops=2 * n_all * d_model * width, bytes_accessed=2 * n_all * d_model + 2 * d_model * width, transcendentals=0),
    )(normed, w_q, cos_t.reshape(n_all, HEAD_DIM), sin_t.reshape(n_all, HEAD_DIM))


def d_attn_kernel(dy_ref, w_ref, o_ref, da_ref, dl_ref):
    chunk = HEAD_DIM
    d_all = dotf(dy_ref[...], w_ref[...], NT).astype(BF16)
    da_ref[...] = d_all
    for g in range(d_all.shape[1] // HEAD_DIM):
        cols = slice(g * HEAD_DIM, (g + 1) * HEAD_DIM)
        prod = (d_all[:, cols].astype(F32) * o_ref[:, cols].astype(F32)).T
        total = all8(jnp.sum(prod, axis=0, keepdims=True))
        for i in range(total.shape[1] // chunk):
            dl_ref[i // 2, i % 2, :, cols] = total[:, i * chunk:(i + 1) * chunk]


def d_attn_of(dy, w_o, o_h, h, tile=512):
    n_all, d_model = dy.shape
    width = o_h.shape[1]
    rows = tile // (2 * HEAD_DIM)
    return pl.pallas_call(
        d_attn_kernel,
        grid=(n_all // tile,),
        in_specs=[
            pl.BlockSpec((tile, d_model), lambda i: (i, 0)),
            pl.BlockSpec((width, d_model), lambda i: (h, 0)),
            pl.BlockSpec((tile, width), lambda i: (i, 0)),
        ],
        out_specs=[
            pl.BlockSpec((tile, width), lambda i: (i, 0)),
            pl.BlockSpec((rows, 2, 8, width), lambda i: (i, 0, 0, 0)),
        ],
        out_shape=[
            jax.ShapeDtypeStruct((n_all, width), BF16),
            jax.ShapeDtypeStruct((n_all // (2 * HEAD_DIM), 2, 8, width), F32),
        ],
        compiler_params=params(),
        cost_estimate=pl.CostEstimate(flops=2 * n_all * d_model * width, bytes_accessed=2 * n_all * d_model + 2 * d_model * width, transcendentals=0),
    )(dy, w_o, o_h)


def pair_list(group):
    return [(2 * j, min(2, group - 2 * j)) for j in range((group + 1) // 2)]


def block_place(b, n_dev):
    half = (b >= n_dev // 2).astype(jnp.int32)
    dev = 2 * jnp.where(half == 1, n_dev - 1 - b, b)
    return dev, half


def block_mask(b, half, lo_row, hi_row):
    key = rows8(lax.broadcasted_iota(jnp.int32, (2 * HEAD_DIM, HEAD_DIM), 0))
    key = (key ^ (half * HEAD_DIM)) + b * (2 * HEAD_DIM)
    return (key >= lo_row) & (key <= hi_row)


def block_list(c, row, lo_sm, full_sm, qc_sm):
    lo, full, last = lo_sm[row, c], full_sm[row, c], qc_sm[c] // 2
    n_plain = last - full
    n_all = n_plain + full - lo + 1

    def block(t):
        m = lo + t - n_plain
        return jnp.where(t < n_plain, full + t, jnp.where(m < full, m, last))

    return n_plain, n_all, block


def attn_fwd_kernel(lo_sm, full_sm, qc_sm, q_ref, kv_ref, lim_ref, o_ref, lse_ref, vt, qs, m_ref, l_ref, acc, s_a, s_b, *, group):
    row = pl.program_id(0)
    n_dev = kv_ref.shape[0]
    chunk = HEAD_DIM

    def key_block(b):
        dev, half = block_place(b, n_dev)
        return kv_ref.at[pl.ds(dev, 2), 0, half, 0]

    def turn(b, carry):
        v = key_block(b)[:, :, HEAD_DIM:].reshape(2 * chunk, HEAD_DIM)
        vt[b] = v.T
        return carry

    lax.fori_loop(jnp.minimum(lo_sm[row, 0], lo_sm[row, 1]), qc_sm[1] // 2 + 1, turn, 0)
    spans = [(slice(g0 * chunk, (g0 + ng) * chunk), ng) for g0, ng in pair_list(group)]
    n_span = len(spans)

    def one_chunk(c, carry):
        base = pl.multiple_of(c * chunk, chunk)
        for g in range(group):
            qs[g * chunk:(g + 1) * chunk, :] = q_ref[pl.ds(base, chunk), g * HEAD_DIM:(g + 1) * HEAD_DIM]
        m_ref[...] = jnp.full_like(m_ref, NEG_BIG)
        l_ref[...] = jnp.zeros_like(l_ref)
        acc[...] = jnp.zeros_like(acc)
        lo_row, hi_row = lim_ref[0, c, 0], lim_ref[0, c, 1]

        def keys_of(b):
            return key_block(b)[:, :, :HEAD_DIM].reshape(2 * chunk, HEAD_DIM)

        def step(now, later, b, b_next, keep):
            k = keys_of(b_next)
            v_t = vt[b]

            def score(j):
                cols = spans[j][0]
                later[:, cols] = dotf(k, qs[cols, :], NT)

            if keep is not None:
                _, half = block_place(b, n_dev)
                ok = block_mask(b, half, lo_row, hi_row) & keep
            score(0)
            for j, (cols, ng) in enumerate(spans):
                if j + 1 < n_span:
                    score(j + 1)
                s = rows8(now[:, cols])
                if keep is not None:
                    s = jnp.concatenate([jnp.where(ok, s[:, :, i * chunk:(i + 1) * chunk], NEG_BIG) for i in range(ng)], axis=2)
                m_old = m_ref[:, cols]
                m_new = jnp.maximum(m_old, all8(jnp.max(jnp.max(s, axis=0), axis=0, keepdims=True)))
                p = jnp.exp2((s - m_new) * SCALE2)
                alpha = jnp.exp2((m_old - m_new) * SCALE2)
                m_ref[:, cols] = m_new
                l_ref[:, cols] = l_ref[:, cols] * alpha + jnp.sum(p, axis=0)
                acc[:, cols] = rows8(rows8(acc[:, cols]) * alpha) + dotf(v_t, rows8(p).astype(BF16), NN)

        n_plain, n_all, block = block_list(c, row, lo_sm, full_sm, qc_sm)
        k0 = keys_of(block(0))
        for cols, _ in spans:
            s_a[:, cols] = dotf(k0, qs[cols, :], NT)

        def pair(use_mask):
            def one(i, carry):
                t = 2 * i
                step(s_a, s_b, block(t), block(t + 1), t < n_all if use_mask else None)
                step(s_b, s_a, block(t + 1), block(t + 2), t + 1 < n_all if use_mask else None)
                return carry

            return one

        lax.fori_loop(0, n_plain // 2, pair(False), 0)
        lax.fori_loop(n_plain // 2, (n_all + 1) // 2, pair(True), 0)
        l_all = all8(jnp.sum(l_ref[...], axis=0, keepdims=True))
        inv_l = 1.0 / l_all
        lse_ref[0, c] = m_ref[...] * SCALE2 + jnp.log(l_all) * LOG2E
        for g in range(group):
            cols = slice(g * chunk, (g + 1) * chunk)
            o_t = rows8(rows8(acc[:, cols]) * inv_l[:, cols])
            o_ref[pl.ds(base, chunk), cols] = o_t.T.astype(BF16)
        return carry

    lax.fori_loop(0, 2, one_chunk, 0)


def attn_cost(n_rows, n_dev, width, n_mat):
    pairs = n_rows * (2 * n_dev + 1) * 128 * 128 * (width // HEAD_DIM)
    return pl.CostEstimate(flops=4 * n_mat * pairs * HEAD_DIM, bytes_accessed=8 * n_rows * 256 * width, transcendentals=pairs)


def attn_fwd(scalars, q, kv, at, limits):
    n_all, width = q.shape
    n_dev, _, _, n_rows, chunk, _ = kv.shape
    group = width // HEAD_DIM
    n_tok = n_all // n_rows
    return pl.pallas_call(
        functools.partial(attn_fwd_kernel, group=group),
        grid_spec=pltpu.PrefetchScalarGridSpec(
            num_scalar_prefetch=3,
            grid=(n_rows,),
            in_specs=[
                pl.BlockSpec((n_tok, width), lambda i, *_: (i, 0)),
                pl.BlockSpec((n_dev, 1, 2, 1, chunk, 2 * HEAD_DIM), lambda i, *_: (0, at, 0, i, 0, 0)),
                pl.BlockSpec((1, 2, 2, 8, chunk), lambda i, *_: (i, 0, 0, 0, 0)),
            ],
            out_specs=[
                pl.BlockSpec((n_tok, width), lambda i, *_: (i, 0)),
                pl.BlockSpec((1, 2, 8, width), lambda i, *_: (i, 0, 0, 0)),
            ],
            scratch_shapes=[
                pltpu.VMEM((n_dev, HEAD_DIM, 2 * chunk), BF16),
                pltpu.VMEM((group * chunk, HEAD_DIM), BF16),
                pltpu.VMEM((8, width), F32),
                pltpu.VMEM((8, width), F32),
                pltpu.VMEM((HEAD_DIM, width), F32),
                pltpu.VMEM((2 * chunk, width), F32),
                pltpu.VMEM((2 * chunk, width), F32),
            ],
        ),
        out_shape=[
            jax.ShapeDtypeStruct((n_all, width), BF16),
            jax.ShapeDtypeStruct((n_rows, 2, 8, width), F32),
        ],
        compiler_params=params(),
        cost_estimate=attn_cost(n_rows, n_dev, width, 2),
    )(*scalars, q, kv, limits)


def attn_bwd_kernel(lo_sm, full_sm, qc_sm, q_ref, kv_ref, lim_ref, do_ref, lse_ref, dl_ref, cos_ref, sin_ref, dq_ref, keep_ref, send_ref, kt, qs, dos, dqt, dkv_ref, s_a, s_b, d_a, d_b, *, group):
    row = pl.program_id(0)
    n_dev = kv_ref.shape[0]
    chunk = HEAD_DIM
    dkv_ref[...] = jnp.zeros_like(dkv_ref)

    def key_block(b):
        dev, half = block_place(b, n_dev)
        return kv_ref.at[pl.ds(dev, 2), 0, half, 0]

    def turn(b, carry):
        k = key_block(b)[:, :, :HEAD_DIM].reshape(2 * chunk, HEAD_DIM)
        kt[b] = k.T
        return carry

    lax.fori_loop(jnp.minimum(lo_sm[row, 0], lo_sm[row, 1]), qc_sm[1] // 2 + 1, turn, 0)
    spans = [(slice(g0 * chunk, (g0 + ng) * chunk), ng) for g0, ng in pair_list(group)]

    def one_chunk(c, carry):
        base = pl.multiple_of(c * chunk, chunk)
        for g in range(group):
            cols = slice(g * HEAD_DIM, (g + 1) * HEAD_DIM)
            qs[g * chunk:(g + 1) * chunk, :] = q_ref[pl.ds(base, chunk), cols]
            dos[g * chunk:(g + 1) * chunk, :] = do_ref[pl.ds(base, chunk), cols]
        dqt[...] = jnp.zeros_like(dqt)
        lo_row, hi_row = lim_ref[0, c, 0], lim_ref[0, c, 1]

        def keys_of(b):
            kv = key_block(b)[...].reshape(2 * chunk, 2 * HEAD_DIM)
            return kv[:, :HEAD_DIM], kv[:, HEAD_DIM:]

        def score(later, k, v, j):
            cols = spans[j][0]
            later[0][:, cols] = dotf(k, qs[cols, :], NT)
            later[1][:, cols] = dotf(v, dos[cols, :], NT)

        def step(now, later, b, b_next, keep):
            dev, half = block_place(b, n_dev)
            k_next, v_next = keys_of(b_next)
            k_t = kt[b]
            if keep is not None:
                ok = block_mask(b, half, lo_row, hi_row) & keep
            dk = jnp.zeros((2 * chunk, HEAD_DIM), F32)
            dv = jnp.zeros((2 * chunk, HEAD_DIM), F32)
            score(later, k_next, v_next, 0)
            for j, (cols, ng) in enumerate(spans):
                if j + 1 < len(spans):
                    score(later, k_next, v_next, j + 1)
                p = jnp.exp2(rows8(now[0][:, cols]) * SCALE2 - lse_ref[0, c, :, cols])
                if keep is not None:
                    p = jnp.concatenate([jnp.where(ok, p[:, :, i * chunk:(i + 1) * chunk], 0.0) for i in range(ng)], axis=2)
                ds = rows8(p * (rows8(now[1][:, cols]) - dl_ref[0, c, :, cols])).astype(BF16)
                dv = dv + dotf(rows8(p).astype(BF16), dos[cols, :], NN)
                dk = dk + dotf(ds, qs[cols, :], NN)
                dqt[:, cols] += dotf(k_t, ds, NN)
            out = dkv_ref.at[pl.ds(dev, 2), half]
            out[:, :, :HEAD_DIM] += (dk * SCALE).reshape(2, chunk, HEAD_DIM)
            out[:, :, HEAD_DIM:] += dv.reshape(2, chunk, HEAD_DIM)

        n_plain, n_all, block = block_list(c, row, lo_sm, full_sm, qc_sm)
        even, odd = (s_a, d_a), (s_b, d_b)
        k0, v0 = keys_of(block(0))
        for j in range(len(spans)):
            score(even, k0, v0, j)

        def pair(use_mask):
            def one(i, carry):
                t = 2 * i
                step(even, odd, block(t), block(t + 1), t < n_all if use_mask else None)
                step(odd, even, block(t + 1), block(t + 2), t + 1 < n_all if use_mask else None)
                return carry

            return one

        lax.fori_loop(0, n_plain // 2, pair(False), 0)
        lax.fori_loop(n_plain // 2, (n_all + 1) // 2, pair(True), 0)
        cos_t, sin_t = cos_ref[0, c], sin_ref[0, c]
        for g in range(group):
            cols = slice(g * chunk, (g + 1) * chunk)
            d = dqt[:, cols] * SCALE
            a, b = d[:HEAD_DIM // 2], d[HEAD_DIM // 2:]
            turned = jnp.concatenate([a * cos_t + b * sin_t, b * cos_t - a * sin_t], axis=0)
            dq_ref[pl.ds(base, chunk), cols] = turned.T.astype(BF16)
        return carry

    lax.fori_loop(0, 2, one_chunk, 0)
    core = qc_sm[2]
    for i in range(n_dev // 2):
        for half in range(2):
            keep_ref[i, half, 0] = dkv_ref[2 * i + core, half]
            send_ref[i, half, 0] = dkv_ref[2 * i + 1 - core, half]


def attn_bwd(scalars, q, kv, at, limits, d_o, lse, delta, cos_c, sin_c):
    n_all, width = q.shape
    n_dev, _, _, n_rows, chunk, _ = kv.shape
    group = width // HEAD_DIM
    n_tok = n_all // n_rows
    tok = pl.BlockSpec((n_tok, width), lambda i, *_: (i, 0))
    kvs = pl.BlockSpec((n_dev, 1, 2, 1, chunk, 2 * HEAD_DIM), lambda i, *_: (0, at, 0, i, 0, 0))
    dkvs = pl.BlockSpec((n_dev // 2, 2, 1, chunk, 2 * HEAD_DIM), lambda i, *_: (0, 0, i, 0, 0))
    stat = pl.BlockSpec((1, 2, 8, width), lambda i, *_: (i, 0, 0, 0))
    rope = pl.BlockSpec((1, 2, HEAD_DIM // 2, chunk), lambda i, *_: (i, 0, 0, 0))
    return pl.pallas_call(
        functools.partial(attn_bwd_kernel, group=group),
        grid_spec=pltpu.PrefetchScalarGridSpec(
            num_scalar_prefetch=3,
            grid=(n_rows,),
            in_specs=[tok, kvs, pl.BlockSpec((1, 2, 2, 8, chunk), lambda i, *_: (i, 0, 0, 0, 0)), tok, stat, stat, rope, rope],
            out_specs=[tok, dkvs, dkvs],
            scratch_shapes=[
                pltpu.VMEM((n_dev, HEAD_DIM, 2 * chunk), BF16),
                pltpu.VMEM((group * chunk, HEAD_DIM), BF16),
                pltpu.VMEM((group * chunk, HEAD_DIM), BF16),
                pltpu.VMEM((HEAD_DIM, width), F32),
                pltpu.VMEM((n_dev, 2, chunk, 2 * HEAD_DIM), F32),
            ] + [pltpu.VMEM((2 * chunk, width), F32)] * 4,
        ),
        out_shape=[jax.ShapeDtypeStruct((n_all, width), BF16)]
        + [jax.ShapeDtypeStruct((n_dev // 2, 2, n_rows, chunk, 2 * HEAD_DIM), F32)] * 2,
        compiler_params=params(),
        cost_estimate=attn_cost(n_rows, n_dev, width, 5),
    )(*scalars, q, kv, limits, d_o, lse, delta, cos_c, sin_c)


def sum_core_kernel(at_sm, keep_ref, got_ref, kx_ref, sx_ref, ky_ref, sy_ref):
    x, y = at_sm[0], at_sm[1]
    for i in range(2):
        for o_ref, j in ((kx_ref, x), (sx_ref, 1 - x)):
            o_ref[i, 0] = keep_ref[i, j, 0, 0] + got_ref[i, j, 0, 0]
        for o_ref, j in ((ky_ref, y), (sy_ref, 1 - y)):
            o_ref[i, 0] = keep_ref[j, i, 1, 0] + got_ref[j, i, 1, 0]


def sum_core(at, keep, got):
    shape = keep.shape[3:]
    cells = pl.BlockSpec((2, 2, 2, 1) + shape[1:], lambda i, *_: (0, 0, 0, i, 0, 0))
    pair = pl.BlockSpec((2, 1) + shape[1:], lambda i, *_: (0, i, 0, 0))
    return pl.pallas_call(
        sum_core_kernel,
        grid_spec=pltpu.PrefetchScalarGridSpec(num_scalar_prefetch=1, grid=(shape[0],), in_specs=[cells] * 2, out_specs=[pair] * 4),
        out_shape=[jax.ShapeDtypeStruct((2,) + shape, F32)] * 4,
        compiler_params=params(),
        cost_estimate=pl.CostEstimate(flops=8 * keep.size, bytes_accessed=12 * keep.size, transcendentals=0),
        name="sum_core",
    )(at, keep, got)


def sum_axis_kernel(at_sm, kx_ref, rx_ref, ky_ref, ry_ref, k1_ref, s1_ref, k2_ref, s2_ref):
    x, y = at_sm[0], at_sm[1]
    for o_ref, j in ((k1_ref, y), (s1_ref, 1 - y)):
        o_ref[0] = kx_ref[j, 0] + rx_ref[j, 0]
    for o_ref, j in ((k2_ref, x), (s2_ref, 1 - x)):
        o_ref[0] = ky_ref[j, 0] + ry_ref[j, 0]


def sum_axis(at, kx, rx, ky, ry):
    shape = kx.shape[1:]
    pair = pl.BlockSpec((2, 1) + shape[1:], lambda i, *_: (0, i, 0, 0))
    one = pl.BlockSpec((1,) + shape[1:], lambda i, *_: (i, 0, 0))
    return pl.pallas_call(
        sum_axis_kernel,
        grid_spec=pltpu.PrefetchScalarGridSpec(num_scalar_prefetch=1, grid=(shape[0],), in_specs=[pair] * 4, out_specs=[one] * 4),
        out_shape=[jax.ShapeDtypeStruct(shape, F32)] * 4,
        compiler_params=params(),
        cost_estimate=pl.CostEstimate(flops=8 * kx.size, bytes_accessed=24 * kx.size, transcendentals=0),
        name="sum_axis",
    )(at, kx, rx, ky, ry)


def sum_last_kernel(cos_ref, sin_ref, *refs):
    *in_refs, o_ref = refs
    chunk = HEAD_DIM
    for h in range(len(in_refs) // 4):
        for half in range(2):
            a_ref, b_ref = in_refs[4 * h + 2 * half], in_refs[4 * h + 2 * half + 1]
            rows = slice(half * chunk, (half + 1) * chunk)
            total = a_ref[0] + b_ref[0]
            dk = total[:, :HEAD_DIM]
            dk = dk * cos_ref[0, rows] - pltpu.roll(dk, HEAD_DIM // 2, 1) * sin_ref[0, rows]
            at_k, at_v = h * HEAD_DIM, o_ref.shape[1] // 2 + h * HEAD_DIM
            o_ref[rows, at_k:at_k + HEAD_DIM] = dk.astype(BF16)
            o_ref[rows, at_v:at_v + HEAD_DIM] = total[:, HEAD_DIM:].astype(BF16)


def sum_last(cos_t, sin_t, parts):
    n_rows, n_tok, _ = cos_t.shape
    shape = parts[0].shape
    rope = pl.BlockSpec((1, n_tok, HEAD_DIM), lambda i: (i, 0, 0))
    one = pl.BlockSpec((1,) + shape[1:], lambda i: (i, 0, 0))
    cols = len(parts) // 4 * shape[2]
    return pl.pallas_call(
        sum_last_kernel,
        grid=(n_rows,),
        in_specs=[rope] * 2 + [one] * len(parts),
        out_specs=pl.BlockSpec((n_tok, cols), lambda i: (i, 0)),
        out_shape=jax.ShapeDtypeStruct((n_rows * n_tok, cols), BF16),
        compiler_params=params(),
        cost_estimate=pl.CostEstimate(flops=8 * parts[0].size * len(parts), bytes_accessed=4 * parts[0].size * len(parts), transcendentals=0),
        name="sum_last",
    )(cos_t, sin_t, *parts)


def copy_kernel(i_ref, o_ref):
    o_ref[...] = i_ref[...].reshape(o_ref.shape)


def split_kernel(i_ref, k_ref, v_ref):
    k_ref[...] = i_ref[0, :, :k_ref.shape[1]]
    v_ref[...] = i_ref[0, :, k_ref.shape[1]:]


def place(x, grid, in_spec, outs, kernel=copy_kernel):
    return pl.pallas_call(
        kernel,
        grid=grid,
        in_specs=[in_spec],
        out_specs=[spec for _, spec in outs],
        out_shape=[jax.ShapeDtypeStruct(shape, x.dtype) for shape, _ in outs],
        compiler_params=params(),
        cost_estimate=pl.CostEstimate(flops=x.size, bytes_accessed=8 * x.size, transcendentals=0),
    )(x)


def solution(mesh):
    n_dev = mesh.shape['cp']

    def block(hidden, grad_out, positions, seg_ids, w_q, w_k, w_v, w_o, norm_gain):
        n_batch, n_tok, d_model = hidden.shape
        n_all = n_batch * n_tok
        chunk = n_tok // 2
        kv_heads = w_k.shape[1] // HEAD_DIM
        width = w_q.shape[1] // kv_heads
        heads = range(kv_heads)
        rank = lax.axis_index('cp')

        q_chunks = jnp.stack([rank, 2 * n_dev - 1 - rank, rank & 1]).astype(jnp.int32)
        glob = (q_chunks[:2, None] * chunk + jnp.arange(chunk, dtype=jnp.int32)[None, :])
        pos_c = positions.reshape(n_batch, 2, chunk)
        doc_start = glob[None] - pos_c
        limits = jnp.stack([doc_start, jnp.broadcast_to(glob[None], doc_start.shape)], axis=2)
        limits = jnp.broadcast_to(limits[:, :, :, None], (n_batch, 2, 2, 8, chunk))
        blk = 2 * chunk
        last = q_chunks[:2] // 2
        lo_blk = doc_start[:, :, 0] // blk
        full_blk = jnp.minimum((doc_start[:, :, -1] + blk - 1) // blk, last[None, :])
        scalars = (lo_blk, full_blk, q_chunks)

        inv_freq = ROPE_BASE ** (-jnp.arange(0, HEAD_DIM, 2).astype(F32) / HEAD_DIM)
        pos_f = positions.astype(F32)
        ang = pos_f[..., None] * inv_freq
        cos_h, sin_h = jnp.cos(ang), jnp.sin(ang)
        cos_t = jnp.concatenate([cos_h, cos_h], axis=-1)
        sin_t = jnp.concatenate([-sin_h, sin_h], axis=-1)
        cos_c = jnp.swapaxes(cos_h.reshape(n_batch, 2, chunk, HEAD_DIM // 2), 2, 3)
        sin_c = jnp.swapaxes(sin_h.reshape(n_batch, 2, chunk, HEAD_DIM // 2), 2, 3)

        cos_t, sin_t = lax.optimization_barrier((cos_t, sin_t))
        core, at = rank & 1, jnp.stack([(rank >> 1) & 1, (rank >> 2) & 1]).astype(jnp.int32)

        def send(value, bit):
            return lax.ppermute(value, 'cp', [(i, i ^ bit) for i in range(n_dev)])

        def half_cols(value, which):
            return lax.dynamic_slice_in_dim(value, which * (d_model // 2), d_model // 2, 1)

        same_core = [[i + j for i in range(0, n_dev, 2)] for j in range(2)]
        scatter = functools.partial(lax.psum_scatter, axis_name='cp', scatter_dimension=0, axis_index_groups=same_core, tiled=True)
        gather = functools.partial(lax.all_gather, axis_name='cp', axis=0, tiled=False)

        normed, *kv_loc = norm_kv(hidden, norm_gain, w_k, w_v, cos_t, sin_t)
        kv_parts = []
        for part in kv_loc:
            kv_parts.append(gather(part))
        kv_of = [(kv_parts[0], 0)] + [(kv_parts[-1], h - 1) for h in heads[1:]]

        dy = grad_out.reshape(n_all, d_model)
        dy_own, dy_pair = half_cols(dy, core), send(half_cols(dy, 1 - core), 1)
        n_own, n_pair = half_cols(normed, core), send(half_cols(normed, 1 - core), 1)
        q, attn, lse, gwo, d_attn, delta = [], [], [], [], [], []
        for h in heads:
            q.append(q_proj(normed, w_q, cos_t, sin_t, h, width))
            o_h, lse_h = attn_fwd(scalars, q[h], *kv_of[h], limits)
            attn.append(o_h)
            lse.append(lse_h)
            o_pair = send(o_h, 1)
            part = dotf(o_h, dy_own, TN)
            part = part + dotf(o_pair, dy_pair, TN)
            gwo.append(scatter(part))
            d_attn_h, delta_h = d_attn_of(dy, w_o, o_h, h)
            d_attn.append(d_attn_h)
            delta.append(delta_h)

        dq, dkv, gwq = [], [], []
        for h in heads:
            dq_h, keep, give = attn_bwd(scalars, q[h], *kv_of[h], limits, d_attn[h], lse[h], delta[h], cos_c, sin_c)
            dq.append(dq_h)
            dq_pair = send(dq_h, 1)
            part = dotf(n_own, dq_h, TN)
            part = part + dotf(n_pair, dq_pair, TN)
            gwq.append(scatter(part))
            got = send(give, 1)
            cells = (2, 2) + keep.shape[1:]
            kx, sx, ky, sy = sum_core(at, keep.reshape(cells), got.reshape(cells))
            rx, ry = send(sx, 2), send(sy, 4)
            k1, s1, k2, s2 = sum_axis(at, kx, rx, ky, ry)
            dkv += [k1, send(s1, 4), k2, send(s2, 2)]
        gwo_all = gather(jnp.stack(gwo))

        attn_flat = jnp.concatenate(attn, axis=1)
        proj_out = dotf(attn_flat, w_o, NN).reshape(hidden.shape)
        block_out = (hidden.astype(F32) + proj_out).astype(BF16)
        dq_flat = jnp.concatenate(dq, axis=1)
        d_norm_q = dotf(dq_flat, w_q, NT)

        dkv_lin = sum_last(cos_t, sin_t, dkv)
        dkv_pair = send(dkv_lin, 1)
        part = dotf(n_own, dkv_lin, TN)
        part = part + dotf(n_pair, dkv_pair, TN)
        gwkv = scatter(part)
        gwq_all = gather(jnp.concatenate(gwq, axis=1))

        w_kv = jnp.concatenate([w_k, w_v], axis=1)
        d_norm_kv = dotf(dkv_lin, w_kv, NT)
        d_normed = (d_norm_q + d_norm_kv).astype(BF16).astype(F32)
        x = hidden.astype(F32).reshape(n_all, d_model)
        inv = lax.rsqrt(jnp.mean(x * x, axis=-1, keepdims=True) + NORM_EPS)
        xn = x * inv
        u = d_normed * norm_gain.astype(F32)
        d_x = inv * (u - xn * jnp.mean(u * xn, axis=-1, keepdims=True))
        grad_hidden = (dy.astype(F32) + d_x).astype(BF16).reshape(hidden.shape)
        grad_gain = lax.psum(jnp.sum(d_normed * xn, axis=0), 'cp')
        gwkv_all = gather(gwkv)

        n_chip = n_dev // 2
        rows_o, rows_q = width // n_chip, d_model // n_dev
        grad_wo, = place(
            gwo_all, (n_dev, kv_heads), pl.BlockSpec((1, 1, rows_o, d_model // 2), lambda d, h: (d, h, 0, 0)),
            [(w_o.shape, pl.BlockSpec((rows_o, d_model // 2), lambda d, h: (h * n_chip + d // 2, d % 2)))])
        gwq_all, grad_hidden, grad_gain = lax.optimization_barrier((gwq_all, grad_hidden, grad_gain))
        at_q = lambda d: ((d % 2) * n_chip + d // 2, 0)
        grad_wq, = place(
            gwq_all, (n_dev,), pl.BlockSpec((1, rows_q, w_q.shape[1]), lambda d: (d, 0, 0)),
            [(w_q.shape, pl.BlockSpec((rows_q, w_q.shape[1]), at_q))])
        grad_wk, grad_wv = place(
            gwkv_all, (n_dev,), pl.BlockSpec((1, rows_q, 2 * w_k.shape[1]), lambda d: (d, 0, 0)),
            [(w_k.shape, pl.BlockSpec((rows_q, w_k.shape[1]), at_q))] * 2, split_kernel)
        return block_out, grad_hidden, grad_wq, grad_wk, grad_wv, grad_wo, grad_gain

    seq_spec = P(None, 'cp', None)
    tok_spec = P(None, 'cp')
    full = P()
    return jax.shard_map(block, mesh=mesh, in_specs=(seq_spec, seq_spec, tok_spec, tok_spec, full, full, full, full, full), out_specs=(seq_spec, seq_spec, full, full, full, full, full), check_vma=False)
```

```python
import functools
import math

import jax
import jax.numpy as jnp
from jax import lax
from jax.experimental import pallas as pl
from jax.experimental.pallas import tpu as pltpu
from jax.sharding import PartitionSpec as P


HEAD_DIM = 128
NORM_EPS = 1e-5
ROPE_BASE = 500000.0
NEG_BIG = -1e30
SCALE = HEAD_DIM ** -0.5
LOG2E = math.log2(math.e)
SCALE2 = SCALE * LOG2E
BF16 = jnp.bfloat16
F32 = jnp.float32
VMEM_LIMIT = 60 * 1024 * 1024
NT = (((1,), (1,)), ((), ()))
NN = (((1,), (0,)), ((), ()))
TN = (((0,), (0,)), ((), ()))


def dotf(a, b, dims):
    return lax.dot_general(a, b, dims, preferred_element_type=F32)


def rows8(x):
    return x.reshape(x.shape[0] // 8, 8, x.shape[1]) if x.ndim == 2 else x.reshape(x.shape[0] * 8, x.shape[2])


def all8(x):
    return jnp.broadcast_to(x, (8, x.shape[1]))


def params(**kw):
    return pltpu.CompilerParams(vmem_limit_bytes=VMEM_LIMIT, **kw)


def norm_kv_kernel(x_ref, g_ref, wk_ref, wv_ref, cos_ref, sin_ref, n_ref, *kv_refs):
    n_tok = x_ref.shape[1]
    half = n_tok // 2
    x = x_ref[0].astype(F32)
    inv = lax.rsqrt(jnp.mean(x * x, axis=-1, keepdims=True) + NORM_EPS)
    normed = rows8(rows8(x * inv) * g_ref[...]).astype(BF16)
    n_ref[...] = normed
    k_all = dotf(normed, wk_ref[...], NN)
    v_all = dotf(normed, wv_ref[...], NN)
    cos_t, sin_t = cos_ref[0], sin_ref[0]
    for h in range(wk_ref.shape[1] // HEAD_DIM):
        kv_ref, at = (kv_refs[0], 0) if h == 0 else (kv_refs[1], h - 1)
        cols = slice(h * HEAD_DIM, (h + 1) * HEAD_DIM)
        k = k_all[:, cols]
        k = (k * cos_t + pltpu.roll(k, HEAD_DIM // 2, 1) * sin_t).astype(BF16)
        v = v_all[:, cols].astype(BF16)
        for i in range(2):
            kv_ref[at, i, 0, :, :HEAD_DIM] = k[i * half:(i + 1) * half]
            kv_ref[at, i, 0, :, HEAD_DIM:] = v[i * half:(i + 1) * half]


def norm_kv(hidden, gain, w_k, w_v, cos_t, sin_t):
    n_batch, n_tok, d_model = hidden.shape
    kv_heads = w_k.shape[1] // HEAD_DIM
    half = n_tok // 2
    row = pl.BlockSpec((1, n_tok, HEAD_DIM), lambda i: (i, 0, 0))
    whole = pl.BlockSpec(w_k.shape, lambda i: (0, 0))
    parts = [1, kv_heads - 1] if kv_heads > 1 else [1]
    return pl.pallas_call(
        norm_kv_kernel,
        grid=(n_batch,),
        in_specs=[
            pl.BlockSpec((1, n_tok, d_model), lambda i: (i, 0, 0)),
            pl.BlockSpec((8, d_model), lambda i: (0, 0)),
            whole, whole, row, row,
        ],
        out_specs=[pl.BlockSpec((n_tok, d_model), lambda i: (i, 0))]
        + [pl.BlockSpec((n, 2, 1, half, 2 * HEAD_DIM), lambda i: (0, 0, i, 0, 0)) for n in parts],
        out_shape=[jax.ShapeDtypeStruct((n_batch * n_tok, d_model), BF16)]
        + [jax.ShapeDtypeStruct((n, 2, n_batch, half, 2 * HEAD_DIM), BF16) for n in parts],
        compiler_params=params(),
        cost_estimate=pl.CostEstimate(flops=4 * n_batch * n_tok * d_model * w_k.shape[1], bytes_accessed=4 * hidden.size + 4 * w_k.size, transcendentals=0),
        name="norm_kv",
    )(hidden, jnp.broadcast_to(gain.astype(F32), (8, d_model)), w_k, w_v, cos_t, sin_t)


def q_proj_kernel(n_ref, w_ref, cos_ref, sin_ref, q_ref):
    q = dotf(n_ref[...], w_ref[...], NN)
    cos_t, sin_t = cos_ref[...], sin_ref[...]
    for g in range(q.shape[1] // HEAD_DIM):
        cols = slice(g * HEAD_DIM, (g + 1) * HEAD_DIM)
        qg = q[:, cols]
        q_ref[:, cols] = (qg * cos_t + pltpu.roll(qg, HEAD_DIM // 2, 1) * sin_t).astype(BF16)


def q_proj(normed, w_q, cos_t, sin_t, h, width, tile=512):
    n_all, d_model = normed.shape
    return pl.pallas_call(
        q_proj_kernel,
        grid=(n_all // tile,),
        in_specs=[
            pl.BlockSpec((tile, d_model), lambda i: (i, 0)),
            pl.BlockSpec((d_model, width), lambda i: (0, h)),
            pl.BlockSpec((tile, HEAD_DIM), lambda i: (i, 0)),
            pl.BlockSpec((tile, HEAD_DIM), lambda i: (i, 0)),
        ],
        out_specs=pl.BlockSpec((tile, width), lambda i: (i, 0)),
        out_shape=jax.ShapeDtypeStruct((n_all, width), BF16),
        compiler_params=params(),
        cost_estimate=pl.CostEstimate(flops=2 * n_all * d_model * width, bytes_accessed=2 * n_all * d_model + 2 * d_model * width, transcendentals=0),
    )(normed, w_q, cos_t.reshape(n_all, HEAD_DIM), sin_t.reshape(n_all, HEAD_DIM))


def d_attn_kernel(dy_ref, w_ref, o_ref, da_ref, dl_ref):
    chunk = HEAD_DIM
    d_all = dotf(dy_ref[...], w_ref[...], NT).astype(BF16)
    da_ref[...] = d_all
    for g in range(d_all.shape[1] // HEAD_DIM):
        cols = slice(g * HEAD_DIM, (g + 1) * HEAD_DIM)
        prod = (d_all[:, cols].astype(F32) * o_ref[:, cols].astype(F32)).T
        total = all8(jnp.sum(prod, axis=0, keepdims=True))
        for i in range(total.shape[1] // chunk):
            dl_ref[i // 2, i % 2, :, cols] = total[:, i * chunk:(i + 1) * chunk]


def d_attn_of(dy, w_o, o_h, h, tile=512):
    n_all, d_model = dy.shape
    width = o_h.shape[1]
    rows = tile // (2 * HEAD_DIM)
    return pl.pallas_call(
        d_attn_kernel,
        grid=(n_all // tile,),
        in_specs=[
            pl.BlockSpec((tile, d_model), lambda i: (i, 0)),
            pl.BlockSpec((width, d_model), lambda i: (h, 0)),
            pl.BlockSpec((tile, width), lambda i: (i, 0)),
        ],
        out_specs=[
            pl.BlockSpec((tile, width), lambda i: (i, 0)),
            pl.BlockSpec((rows, 2, 8, width), lambda i: (i, 0, 0, 0)),
        ],
        out_shape=[
            jax.ShapeDtypeStruct((n_all, width), BF16),
            jax.ShapeDtypeStruct((n_all // (2 * HEAD_DIM), 2, 8, width), F32),
        ],
        compiler_params=params(),
        cost_estimate=pl.CostEstimate(flops=2 * n_all * d_model * width, bytes_accessed=2 * n_all * d_model + 2 * d_model * width, transcendentals=0),
    )(dy, w_o, o_h)


def pair_list(group):
    return [(2 * j, min(2, group - 2 * j)) for j in range((group + 1) // 2)]


def block_place(b, n_dev):
    half = (b >= n_dev // 2).astype(jnp.int32)
    dev = 2 * jnp.where(half == 1, n_dev - 1 - b, b)
    return dev, half


def block_mask(b, half, lo_row, hi_row):
    key = rows8(lax.broadcasted_iota(jnp.int32, (2 * HEAD_DIM, HEAD_DIM), 0))
    key = (key ^ (half * HEAD_DIM)) + b * (2 * HEAD_DIM)
    return (key >= lo_row) & (key <= hi_row)


def block_list(c, row, lo_sm, full_sm, qc_sm):
    lo, full, last = lo_sm[row, c], full_sm[row, c], qc_sm[c] // 2
    n_plain = last - full
    n_all = n_plain + full - lo + 1

    def block(t):
        m = lo + t - n_plain
        return jnp.where(t < n_plain, full + t, jnp.where(m < full, m, last))

    return n_plain, n_all, block


def run_blocks(blocks, first, step, even, odd):
    n_plain, n_all, block = blocks
    first(block(0))

    def pair(use_mask):
        def one(i, carry):
            t = 2 * i
            step(even, odd, block(t), block(t + 1), use_mask)
            step(odd, even, block(t + 1), block(t + 2), use_mask)
            return carry

        return one

    lax.fori_loop(0, n_plain // 2, pair(False), 0)
    lax.fori_loop(n_plain // 2, n_all // 2, pair(True), 0)

    @pl.when(n_all % 2 == 1)
    def _():
        step(even, None, block(n_all - 1), None, True)


def attn_fwd_kernel(lo_sm, full_sm, qc_sm, q_ref, kv_ref, lim_ref, o_ref, lse_ref, vt, qs, m_ref, l_ref, acc, s_a, s_b, *, group):
    row = pl.program_id(0)
    n_dev = kv_ref.shape[0]
    chunk = HEAD_DIM

    def key_block(b):
        dev, half = block_place(b, n_dev)
        return kv_ref.at[pl.ds(dev, 2), 0, half, 0]

    def turn(b, carry):
        v = key_block(b)[:, :, HEAD_DIM:].reshape(2 * chunk, HEAD_DIM)
        vt[b] = v.T
        return carry

    lax.fori_loop(jnp.minimum(lo_sm[row, 0], lo_sm[row, 1]), qc_sm[1] // 2 + 1, turn, 0)
    spans = [(slice(g0 * chunk, (g0 + ng) * chunk), ng) for g0, ng in pair_list(group)]
    n_span = len(spans)

    def one_chunk(c, carry):
        base = pl.multiple_of(c * chunk, chunk)
        for g in range(group):
            qs[g * chunk:(g + 1) * chunk, :] = q_ref[pl.ds(base, chunk), g * HEAD_DIM:(g + 1) * HEAD_DIM]
        m_ref[...] = jnp.full_like(m_ref, NEG_BIG)
        l_ref[...] = jnp.zeros_like(l_ref)
        acc[...] = jnp.zeros_like(acc)
        lo_row, hi_row = lim_ref[0, c, 0], lim_ref[0, c, 1]

        def keys_of(b):
            return key_block(b)[:, :, :HEAD_DIM].reshape(2 * chunk, HEAD_DIM)

        def step(now, later, b, b_next, use_mask):
            v_t = vt[b]

            def score(j):
                if later is not None and j < n_span:
                    cols = spans[j][0]
                    later[:, cols] = dotf(keys_of(b_next), qs[cols, :], NT)

            if use_mask:
                _, half = block_place(b, n_dev)
                ok = block_mask(b, half, lo_row, hi_row)
            score(0)
            for j, (cols, ng) in enumerate(spans):
                score(j + 1)
                s = rows8(now[:, cols])
                if use_mask:
                    s = jnp.concatenate([jnp.where(ok, s[:, :, i * chunk:(i + 1) * chunk], NEG_BIG) for i in range(ng)], axis=2)
                m_old = m_ref[:, cols]
                m_new = jnp.maximum(m_old, all8(jnp.max(jnp.max(s, axis=0), axis=0, keepdims=True)))
                p = jnp.exp2((s - m_new) * SCALE2)
                alpha = jnp.exp2((m_old - m_new) * SCALE2)
                m_ref[:, cols] = m_new
                l_ref[:, cols] = l_ref[:, cols] * alpha + jnp.sum(p, axis=0)
                acc[:, cols] = rows8(rows8(acc[:, cols]) * alpha) + dotf(v_t, rows8(p).astype(BF16), NN)

        def first(b):
            k = keys_of(b)
            for cols, _ in spans:
                s_a[:, cols] = dotf(k, qs[cols, :], NT)

        run_blocks(block_list(c, row, lo_sm, full_sm, qc_sm), first, step, s_a, s_b)
        l_all = all8(jnp.sum(l_ref[...], axis=0, keepdims=True))
        inv_l = 1.0 / l_all
        lse_ref[0, c] = m_ref[...] * SCALE2 + jnp.log(l_all) * LOG2E
        for g in range(group):
            cols = slice(g * chunk, (g + 1) * chunk)
            o_t = rows8(rows8(acc[:, cols]) * inv_l[:, cols])
            o_ref[pl.ds(base, chunk), cols] = o_t.T.astype(BF16)
        return carry

    lax.fori_loop(0, 2, one_chunk, 0)


def attn_cost(n_rows, n_dev, width, n_mat):
    pairs = n_rows * (2 * n_dev + 1) * 128 * 128 * (width // HEAD_DIM)
    return pl.CostEstimate(flops=4 * n_mat * pairs * HEAD_DIM, bytes_accessed=8 * n_rows * 256 * width, transcendentals=pairs)


def attn_fwd(scalars, q, kv, at, limits):
    n_all, width = q.shape
    n_dev, _, _, n_rows, chunk, _ = kv.shape
    group = width // HEAD_DIM
    n_tok = n_all // n_rows
    return pl.pallas_call(
        functools.partial(attn_fwd_kernel, group=group),
        grid_spec=pltpu.PrefetchScalarGridSpec(
            num_scalar_prefetch=3,
            grid=(n_rows,),
            in_specs=[
                pl.BlockSpec((n_tok, width), lambda i, *_: (i, 0)),
                pl.BlockSpec((n_dev, 1, 2, 1, chunk, 2 * HEAD_DIM), lambda i, *_: (0, at, 0, i, 0, 0)),
                pl.BlockSpec((1, 2, 2, 8, chunk), lambda i, *_: (i, 0, 0, 0, 0)),
            ],
            out_specs=[
                pl.BlockSpec((n_tok, width), lambda i, *_: (i, 0)),
                pl.BlockSpec((1, 2, 8, width), lambda i, *_: (i, 0, 0, 0)),
            ],
            scratch_shapes=[
                pltpu.VMEM((n_dev, HEAD_DIM, 2 * chunk), BF16),
                pltpu.VMEM((group * chunk, HEAD_DIM), BF16),
                pltpu.VMEM((8, width), F32),
                pltpu.VMEM((8, width), F32),
                pltpu.VMEM((HEAD_DIM, width), F32),
                pltpu.VMEM((2 * chunk, width), F32),
                pltpu.VMEM((2 * chunk, width), F32),
            ],
        ),
        out_shape=[
            jax.ShapeDtypeStruct((n_all, width), BF16),
            jax.ShapeDtypeStruct((n_rows, 2, 8, width), F32),
        ],
        compiler_params=params(),
        cost_estimate=attn_cost(n_rows, n_dev, width, 2),
    )(*scalars, q, kv, limits)


def attn_bwd_kernel(lo_sm, full_sm, qc_sm, q_ref, kv_ref, lim_ref, do_ref, lse_ref, dl_ref, cos_ref, sin_ref, dq_ref, keep_ref, send_ref, kt, qs, dos, dqt, dkv_ref, s_a, s_b, d_a, d_b, *, group):
    row = pl.program_id(0)
    n_dev = kv_ref.shape[0]
    chunk = HEAD_DIM
    dkv_ref[...] = jnp.zeros_like(dkv_ref)

    def key_block(b):
        dev, half = block_place(b, n_dev)
        return kv_ref.at[pl.ds(dev, 2), 0, half, 0]

    def turn(b, carry):
        k = key_block(b)[:, :, :HEAD_DIM].reshape(2 * chunk, HEAD_DIM)
        kt[b] = k.T
        return carry

    lax.fori_loop(jnp.minimum(lo_sm[row, 0], lo_sm[row, 1]), qc_sm[1] // 2 + 1, turn, 0)
    spans = [(slice(g0 * chunk, (g0 + ng) * chunk), ng) for g0, ng in pair_list(group)]

    def one_chunk(c, carry):
        base = pl.multiple_of(c * chunk, chunk)
        for g in range(group):
            cols = slice(g * HEAD_DIM, (g + 1) * HEAD_DIM)
            qs[g * chunk:(g + 1) * chunk, :] = q_ref[pl.ds(base, chunk), cols]
            dos[g * chunk:(g + 1) * chunk, :] = do_ref[pl.ds(base, chunk), cols]
        dqt[...] = jnp.zeros_like(dqt)
        lo_row, hi_row = lim_ref[0, c, 0], lim_ref[0, c, 1]

        def keys_of(b):
            kv = key_block(b)[...].reshape(2 * chunk, 2 * HEAD_DIM)
            return kv[:, :HEAD_DIM], kv[:, HEAD_DIM:]

        def score(later, k, v, j):
            cols = spans[j][0]
            later[0][:, cols] = dotf(k, qs[cols, :], NT)
            later[1][:, cols] = dotf(v, dos[cols, :], NT)

        def step(now, later, b, b_next, use_mask):
            dev, half = block_place(b, n_dev)
            k_t = kt[b]
            if use_mask:
                ok = block_mask(b, half, lo_row, hi_row)
            dk = jnp.zeros((2 * chunk, HEAD_DIM), F32)
            dv = jnp.zeros((2 * chunk, HEAD_DIM), F32)

            def ahead(j):
                if later is not None and j < len(spans):
                    score(later, *keys_of(b_next), j)

            ahead(0)
            for j, (cols, ng) in enumerate(spans):
                ahead(j + 1)
                p = jnp.exp2(rows8(now[0][:, cols]) * SCALE2 - lse_ref[0, c, :, cols])
                if use_mask:
                    p = jnp.concatenate([jnp.where(ok, p[:, :, i * chunk:(i + 1) * chunk], 0.0) for i in range(ng)], axis=2)
                ds = rows8(p * (rows8(now[1][:, cols]) - dl_ref[0, c, :, cols])).astype(BF16)
                dv = dv + dotf(rows8(p).astype(BF16), dos[cols, :], NN)
                dk = dk + dotf(ds, qs[cols, :], NN)
                dqt[:, cols] += dotf(k_t, ds, NN)
            out = dkv_ref.at[pl.ds(dev, 2), half]
            out[:, :, :HEAD_DIM] += (dk * SCALE).reshape(2, chunk, HEAD_DIM)
            out[:, :, HEAD_DIM:] += dv.reshape(2, chunk, HEAD_DIM)

        def first(b):
            for j in range(len(spans)):
                score((s_a, d_a), *keys_of(b), j)

        run_blocks(block_list(c, row, lo_sm, full_sm, qc_sm), first, step, (s_a, d_a), (s_b, d_b))
        cos_t, sin_t = cos_ref[0, c], sin_ref[0, c]
        for g in range(group):
            cols = slice(g * chunk, (g + 1) * chunk)
            d = dqt[:, cols] * SCALE
            a, b = d[:HEAD_DIM // 2], d[HEAD_DIM // 2:]
            turned = jnp.concatenate([a * cos_t + b * sin_t, b * cos_t - a * sin_t], axis=0)
            dq_ref[pl.ds(base, chunk), cols] = turned.T.astype(BF16)
        return carry

    lax.fori_loop(0, 2, one_chunk, 0)
    core = qc_sm[2]
    for i in range(n_dev // 2):
        for half in range(2):
            keep_ref[i, half, 0] = dkv_ref[2 * i + core, half]
            send_ref[i, half, 0] = dkv_ref[2 * i + 1 - core, half]


def attn_bwd(scalars, q, kv, at, limits, d_o, lse, delta, cos_c, sin_c):
    n_all, width = q.shape
    n_dev, _, _, n_rows, chunk, _ = kv.shape
    group = width // HEAD_DIM
    n_tok = n_all // n_rows
    tok = pl.BlockSpec((n_tok, width), lambda i, *_: (i, 0))
    kvs = pl.BlockSpec((n_dev, 1, 2, 1, chunk, 2 * HEAD_DIM), lambda i, *_: (0, at, 0, i, 0, 0))
    dkvs = pl.BlockSpec((n_dev // 2, 2, 1, chunk, 2 * HEAD_DIM), lambda i, *_: (0, 0, i, 0, 0))
    stat = pl.BlockSpec((1, 2, 8, width), lambda i, *_: (i, 0, 0, 0))
    rope = pl.BlockSpec((1, 2, HEAD_DIM // 2, chunk), lambda i, *_: (i, 0, 0, 0))
    return pl.pallas_call(
        functools.partial(attn_bwd_kernel, group=group),
        grid_spec=pltpu.PrefetchScalarGridSpec(
            num_scalar_prefetch=3,
            grid=(n_rows,),
            in_specs=[tok, kvs, pl.BlockSpec((1, 2, 2, 8, chunk), lambda i, *_: (i, 0, 0, 0, 0)), tok, stat, stat, rope, rope],
            out_specs=[tok, dkvs, dkvs],
            scratch_shapes=[
                pltpu.VMEM((n_dev, HEAD_DIM, 2 * chunk), BF16),
                pltpu.VMEM((group * chunk, HEAD_DIM), BF16),
                pltpu.VMEM((group * chunk, HEAD_DIM), BF16),
                pltpu.VMEM((HEAD_DIM, width), F32),
                pltpu.VMEM((n_dev, 2, chunk, 2 * HEAD_DIM), F32),
            ] + [pltpu.VMEM((2 * chunk, width), F32)] * 4,
        ),
        out_shape=[jax.ShapeDtypeStruct((n_all, width), BF16)]
        + [jax.ShapeDtypeStruct((n_dev // 2, 2, n_rows, chunk, 2 * HEAD_DIM), F32)] * 2,
        compiler_params=params(),
        cost_estimate=attn_cost(n_rows, n_dev, width, 5),
    )(*scalars, q, kv, limits, d_o, lse, delta, cos_c, sin_c)


def grid_spec(n_prefetch, grid, in_specs, out_specs):
    return pltpu.PrefetchScalarGridSpec(num_scalar_prefetch=n_prefetch, grid=grid, in_specs=in_specs, out_specs=out_specs)


def send_parts_kernel(at_sm, px_ref, py_ref, sx_ref, sy_ref):
    sx_ref[0] = px_ref[0, 0, 0]
    sy_ref[0] = py_ref[0, 0, 0]


def send_parts(at, cells):
    rows, cols = cells.shape[3:]
    block = (1, 1, 1, rows, cols)
    out = pl.BlockSpec((1, rows, cols), lambda i, at: (i, 0, 0))
    return pl.pallas_call(
        send_parts_kernel,
        grid_spec=grid_spec(1, (2,), [pl.BlockSpec(block, lambda i, at: (i, 1 - at[0], 0, 0, 0)), pl.BlockSpec(block, lambda i, at: (1 - at[1], i, 1, 0, 0))], [out] * 2),
        out_shape=[jax.ShapeDtypeStruct((2, rows, cols), F32)] * 2,
        compiler_params=params(),
        cost_estimate=pl.CostEstimate(flops=cells.size, bytes_accessed=4 * cells.size, transcendentals=0),
        name="send_parts",
    )(at, cells, cells)


def add_parts_kernel(at_sm, a_ref, b_ref, c_ref, d_ref, ra_ref, rb_ref, rc_ref, rd_ref, *o_refs):
    for o_ref, p_ref, r_ref in zip(o_refs, (a_ref, b_ref, c_ref, d_ref), (ra_ref, rb_ref, rc_ref, rd_ref)):
        o_ref[...] = p_ref[0, 0, 0] + r_ref[0]


def add_parts(at, cells, rx, ry):
    rows, cols = cells.shape[3:]
    n = 2
    block = (1, 1, 1, rows // n, cols)
    got = (1, rows // n, cols)
    part = lambda f: pl.BlockSpec(block, lambda i, at: f(at[0], at[1]) + (i, 0))
    recv = lambda f: pl.BlockSpec(got, lambda i, at: (f(at[0], at[1]), i, 0))
    out = pl.BlockSpec((rows // n, cols), lambda i, at: (i, 0))
    return pl.pallas_call(
        add_parts_kernel,
        grid_spec=grid_spec(1, (n,), [
            part(lambda x, y: (y, x, 0)), part(lambda x, y: (1 - y, x, 0)), part(lambda x, y: (y, x, 1)), part(lambda x, y: (y, 1 - x, 1)),
            recv(lambda x, y: y), recv(lambda x, y: 1 - y), recv(lambda x, y: x), recv(lambda x, y: 1 - x)], [out] * 4),
        out_shape=[jax.ShapeDtypeStruct((rows, cols), F32)] * 4,
        compiler_params=params(),
        cost_estimate=pl.CostEstimate(flops=2 * cells.size, bytes_accessed=6 * cells.size, transcendentals=0),
        name="add_parts",
    )(at, cells, cells, cells, cells, rx, rx, ry, ry)


def add_last_kernel(a_ref, ra_ref, b_ref, rb_ref, o_ref):
    o_ref[0] = a_ref[...] + ra_ref[...]
    o_ref[1] = b_ref[...] + rb_ref[...]


def add_last(k1, r1, k2, r2):
    rows, cols = k1.shape
    n = 2
    one = pl.BlockSpec((rows // n, cols), lambda i: (i, 0))
    return pl.pallas_call(
        add_last_kernel,
        grid=(n,),
        in_specs=[one] * 4,
        out_specs=pl.BlockSpec((2, rows // n, cols), lambda i: (0, i, 0)),
        out_shape=jax.ShapeDtypeStruct((2, rows, cols), F32),
        compiler_params=params(),
        cost_estimate=pl.CostEstimate(flops=2 * k1.size, bytes_accessed=24 * k1.size, transcendentals=0),
        name="add_last",
    )(k1, r1, k2, r2)


def sum_core_kernel(at_sm, keep_ref, got_ref, kx_ref, sx_ref, ky_ref, sy_ref):
    x, y = at_sm[0], at_sm[1]
    for i in range(2):
        for o_ref, j in ((kx_ref, x), (sx_ref, 1 - x)):
            o_ref[i, 0] = keep_ref[i, j, 0, 0] + got_ref[i, j, 0, 0]
        for o_ref, j in ((ky_ref, y), (sy_ref, 1 - y)):
            o_ref[i, 0] = keep_ref[j, i, 1, 0] + got_ref[j, i, 1, 0]


def sum_core(at, keep, got):
    shape = keep.shape[3:]
    cells = pl.BlockSpec((2, 2, 2, 1) + shape[1:], lambda i, *_: (0, 0, 0, i, 0, 0))
    pair = pl.BlockSpec((2, 1) + shape[1:], lambda i, *_: (0, i, 0, 0))
    return pl.pallas_call(
        sum_core_kernel,
        grid_spec=pltpu.PrefetchScalarGridSpec(num_scalar_prefetch=1, grid=(shape[0],), in_specs=[cells] * 2, out_specs=[pair] * 4),
        out_shape=[jax.ShapeDtypeStruct((2,) + shape, F32)] * 4,
        compiler_params=params(),
        cost_estimate=pl.CostEstimate(flops=8 * keep.size, bytes_accessed=12 * keep.size, transcendentals=0),
        name="sum_core",
    )(at, keep, got)


def sum_axis_kernel(at_sm, kx_ref, rx_ref, ky_ref, ry_ref, k1_ref, s1_ref, k2_ref, s2_ref):
    x, y = at_sm[0], at_sm[1]
    for o_ref, j in ((k1_ref, y), (s1_ref, 1 - y)):
        o_ref[0] = kx_ref[j, 0] + rx_ref[j, 0]
    for o_ref, j in ((k2_ref, x), (s2_ref, 1 - x)):
        o_ref[0] = ky_ref[j, 0] + ry_ref[j, 0]


def sum_axis(at, kx, rx, ky, ry):
    shape = kx.shape[1:]
    pair = pl.BlockSpec((2, 1) + shape[1:], lambda i, *_: (0, i, 0, 0))
    one = pl.BlockSpec((1,) + shape[1:], lambda i, *_: (i, 0, 0))
    return pl.pallas_call(
        sum_axis_kernel,
        grid_spec=pltpu.PrefetchScalarGridSpec(num_scalar_prefetch=1, grid=(shape[0],), in_specs=[pair] * 4, out_specs=[one] * 4),
        out_shape=[jax.ShapeDtypeStruct(shape, F32)] * 4,
        compiler_params=params(),
        cost_estimate=pl.CostEstimate(flops=8 * kx.size, bytes_accessed=24 * kx.size, transcendentals=0),
        name="sum_axis",
    )(at, kx, rx, ky, ry)


def sum_last_kernel(cos_ref, sin_ref, *refs):
    *in_refs, o_ref = refs
    chunk = HEAD_DIM
    for h in range(len(in_refs) // 4):
        for half in range(2):
            a_ref, b_ref = in_refs[4 * h + 2 * half], in_refs[4 * h + 2 * half + 1]
            rows = slice(half * chunk, (half + 1) * chunk)
            total = a_ref[0] + b_ref[0]
            dk = total[:, :HEAD_DIM]
            dk = dk * cos_ref[0, rows] - pltpu.roll(dk, HEAD_DIM // 2, 1) * sin_ref[0, rows]
            at_k, at_v = h * HEAD_DIM, o_ref.shape[1] // 2 + h * HEAD_DIM
            o_ref[rows, at_k:at_k + HEAD_DIM] = dk.astype(BF16)
            o_ref[rows, at_v:at_v + HEAD_DIM] = total[:, HEAD_DIM:].astype(BF16)


def sum_last(cos_t, sin_t, parts):
    n_rows, n_tok, _ = cos_t.shape
    shape = parts[0].shape
    rope = pl.BlockSpec((1, n_tok, HEAD_DIM), lambda i: (i, 0, 0))
    one = pl.BlockSpec((1,) + shape[1:], lambda i: (i, 0, 0))
    cols = len(parts) // 4 * shape[2]
    return pl.pallas_call(
        sum_last_kernel,
        grid=(n_rows,),
        in_specs=[rope] * 2 + [one] * len(parts),
        out_specs=pl.BlockSpec((n_tok, cols), lambda i: (i, 0)),
        out_shape=jax.ShapeDtypeStruct((n_rows * n_tok, cols), BF16),
        compiler_params=params(),
        cost_estimate=pl.CostEstimate(flops=8 * parts[0].size * len(parts), bytes_accessed=4 * parts[0].size * len(parts), transcendentals=0),
        name="sum_last",
    )(cos_t, sin_t, *parts)


def copy_kernel(i_ref, *refs):
    o_ref = refs[-1]
    o_ref[...] = i_ref[...].reshape(o_ref.shape)


def split_kernel(i_ref, k_ref, v_ref):
    k_ref[...] = i_ref[0, :, :k_ref.shape[1]]
    v_ref[...] = i_ref[0, :, k_ref.shape[1]:]


def place(x, grid, in_spec, outs, kernel=copy_kernel, into=None):
    return pl.pallas_call(
        kernel,
        grid=grid,
        in_specs=[in_spec] + [pl.BlockSpec(memory_space=pl.ANY)] * (into is not None),
        out_specs=[spec for _, spec in outs],
        out_shape=[jax.ShapeDtypeStruct(shape, x.dtype) for shape, _ in outs],
        input_output_aliases={} if into is None else {1: 0},
        compiler_params=params(),
        cost_estimate=pl.CostEstimate(flops=x.size, bytes_accessed=8 * x.size, transcendentals=0),
    )(*([x] if into is None else [x, into]))


def solution(mesh):
    n_dev = mesh.shape['cp']

    def block(hidden, grad_out, positions, seg_ids, w_q, w_k, w_v, w_o, norm_gain):
        n_batch, n_tok, d_model = hidden.shape
        n_all = n_batch * n_tok
        chunk = n_tok // 2
        kv_heads = w_k.shape[1] // HEAD_DIM
        width = w_q.shape[1] // kv_heads
        heads = range(kv_heads)
        rank = lax.axis_index('cp')

        q_chunks = jnp.stack([rank, 2 * n_dev - 1 - rank, rank & 1]).astype(jnp.int32)
        glob = (q_chunks[:2, None] * chunk + jnp.arange(chunk, dtype=jnp.int32)[None, :])
        pos_c = positions.reshape(n_batch, 2, chunk)
        doc_start = glob[None] - pos_c
        limits = jnp.stack([doc_start, jnp.broadcast_to(glob[None], doc_start.shape)], axis=2)
        limits = jnp.broadcast_to(limits[:, :, :, None], (n_batch, 2, 2, 8, chunk))
        blk = 2 * chunk
        last = q_chunks[:2] // 2
        lo_blk = doc_start[:, :, 0] // blk
        full_blk = jnp.minimum((doc_start[:, :, -1] + blk - 1) // blk, last[None, :])
        scalars = (lo_blk, full_blk, q_chunks)

        inv_freq = ROPE_BASE ** (-jnp.arange(0, HEAD_DIM, 2).astype(F32) / HEAD_DIM)
        pos_f = positions.astype(F32)
        ang = pos_f[..., None] * inv_freq
        cos_h, sin_h = jnp.cos(ang), jnp.sin(ang)
        cos_t = jnp.concatenate([cos_h, cos_h], axis=-1)
        sin_t = jnp.concatenate([-sin_h, sin_h], axis=-1)
        cos_c = jnp.swapaxes(cos_h.reshape(n_batch, 2, chunk, HEAD_DIM // 2), 2, 3)
        sin_c = jnp.swapaxes(sin_h.reshape(n_batch, 2, chunk, HEAD_DIM // 2), 2, 3)

        cos_t, sin_t = lax.optimization_barrier((cos_t, sin_t))
        core, at = rank & 1, jnp.stack([(rank >> 1) & 1, (rank >> 2) & 1]).astype(jnp.int32)

        def send(value, bit):
            return lax.ppermute(value, 'cp', [(i, i ^ bit) for i in range(n_dev)])

        def share(part):
            cells = part.reshape(2, 2, 2, part.shape[0] // 8, part.shape[1])
            sx, sy = send_parts(at, cells)
            rx, ry = send(sx, 2), send(sy, 4)
            k1, s1, k2, s2 = add_parts(at, cells, rx, ry)
            r1, r2 = send(s1, 4), send(s2, 2)
            return add_last(k1, r1, k2, r2).reshape(part.shape[0] // 4, part.shape[1])

        def half_cols(value, which):
            return lax.dynamic_slice_in_dim(value, which * (d_model // 2), d_model // 2, 1)

        same_core = [[i + j for i in range(0, n_dev, 2)] for j in range(2)]
        scatter = functools.partial(lax.psum_scatter, axis_name='cp', scatter_dimension=0, axis_index_groups=same_core, tiled=True)
        gather = functools.partial(lax.all_gather, axis_name='cp', axis=0, tiled=False)

        normed, *kv_loc = norm_kv(hidden, norm_gain, w_k, w_v, cos_t, sin_t)
        kv_parts = []
        for part in kv_loc:
            kv_parts.append(gather(part))
        kv_of = [(kv_parts[0], 0)] + [(kv_parts[-1], h - 1) for h in heads[1:]]

        dy = grad_out.reshape(n_all, d_model)
        dy_own, dy_pair = half_cols(dy, core), send(half_cols(dy, 1 - core), 1)
        n_own, n_pair = half_cols(normed, core), send(half_cols(normed, 1 - core), 1)
        q, attn, lse, gwo, d_attn, delta = [], [], [], [], [], []
        for h in heads:
            q.append(q_proj(normed, w_q, cos_t, sin_t, h, width))
            o_h, lse_h = attn_fwd(scalars, q[h], *kv_of[h], limits)
            attn.append(o_h)
            lse.append(lse_h)
            o_pair = send(o_h, 1)
            part = dotf(o_h, dy_own, TN)
            part = part + dotf(o_pair, dy_pair, TN)
            own = share(part)
            gwo.append(gather(own))
            d_attn_h, delta_h = d_attn_of(dy, w_o, o_h, h)
            d_attn.append(d_attn_h)
            delta.append(delta_h)

        dq, dkv, gwq = [], [], []
        for h in heads:
            dq_h, keep, give = attn_bwd(scalars, q[h], *kv_of[h], limits, d_attn[h], lse[h], delta[h], cos_c, sin_c)
            dq.append(dq_h)
            dq_pair = send(dq_h, 1)
            part = dotf(n_own, dq_h, TN)
            part = part + dotf(n_pair, dq_pair, TN)
            own = share(part)
            gwq.append(gather(own))
            got = send(give, 1)
            cells = (2, 2) + keep.shape[1:]
            kx, sx, ky, sy = sum_core(at, keep.reshape(cells), got.reshape(cells))
            rx, ry = send(sx, 2), send(sy, 4)
            k1, s1, k2, s2 = sum_axis(at, kx, rx, ky, ry)
            dkv += [k1, send(s1, 4), k2, send(s2, 2)]

        attn_flat = jnp.concatenate(attn, axis=1)
        proj_out = dotf(attn_flat, w_o, NN).reshape(hidden.shape)
        block_out = (hidden.astype(F32) + proj_out).astype(BF16)
        dq_flat = jnp.concatenate(dq, axis=1)
        d_norm_q = dotf(dq_flat, w_q, NT)

        dkv_lin = sum_last(cos_t, sin_t, dkv)
        dkv_pair = send(dkv_lin, 1)
        part = dotf(n_own, dkv_lin, TN)
        part = part + dotf(n_pair, dkv_pair, TN)
        gwkv = scatter(part)

        w_kv = jnp.concatenate([w_k, w_v], axis=1)
        d_norm_kv = dotf(dkv_lin, w_kv, NT)
        d_normed = (d_norm_q + d_norm_kv).astype(BF16).astype(F32)
        x = hidden.astype(F32).reshape(n_all, d_model)
        inv = lax.rsqrt(jnp.mean(x * x, axis=-1, keepdims=True) + NORM_EPS)
        xn = x * inv
        u = d_normed * norm_gain.astype(F32)
        d_x = inv * (u - xn * jnp.mean(u * xn, axis=-1, keepdims=True))
        grad_hidden = (dy.astype(F32) + d_x).astype(BF16).reshape(hidden.shape)
        grad_gain = jnp.sum(d_normed * xn, axis=0)
        for bit in (1, 2, 4):
            grad_gain = grad_gain + send(grad_gain, bit)
        gwkv_all = gather(gwkv)

        n_chip = n_dev // 2
        rows_o, rows_q = width // n_chip, d_model // n_dev
        grad_wo = grad_wq = None
        for h in heads:
            grad_wo, = place(
                gwo[h], (n_dev,), pl.BlockSpec((1, rows_o, d_model // 2), lambda d: (d, 0, 0)),
                [(w_o.shape, pl.BlockSpec((rows_o, d_model // 2), lambda d, h=h: (h * n_chip + d // 2, d % 2)))], into=grad_wo)
        at_q = lambda d: ((d % 2) * n_chip + d // 2, 0)
        for h in heads:
            grad_wq, = place(
                gwq[h], (n_dev,), pl.BlockSpec((1, rows_q, width), lambda d: (d, 0, 0)),
                [(w_q.shape, pl.BlockSpec((rows_q, width), lambda d, h=h: (at_q(d)[0], h)))], into=grad_wq)
        grad_wk, grad_wv = place(
            gwkv_all, (n_dev,), pl.BlockSpec((1, rows_q, 2 * w_k.shape[1]), lambda d: (d, 0, 0)),
            [(w_k.shape, pl.BlockSpec((rows_q, w_k.shape[1]), at_q))] * 2, split_kernel)
        return block_out, grad_hidden, grad_wq, grad_wk, grad_wv, grad_wo, grad_gain

    seq_spec = P(None, 'cp', None)
    tok_spec = P(None, 'cp')
    full = P()
    return jax.shard_map(block, mesh=mesh, in_specs=(seq_spec, seq_spec, tok_spec, tok_spec, full, full, full, full, full), out_specs=(seq_spec, seq_spec, full, full, full, full, full), check_vma=False)
```

```python
import functools
import math

import jax
import jax.numpy as jnp
from jax import lax
from jax.experimental import pallas as pl
from jax.experimental.pallas import tpu as pltpu
from jax.sharding import PartitionSpec as P


HEAD_DIM = 128
NORM_EPS = 1e-5
ROPE_BASE = 500000.0
NEG_BIG = -1e30
SCALE = HEAD_DIM ** -0.5
LOG2E = math.log2(math.e)
SCALE2 = SCALE * LOG2E
BF16 = jnp.bfloat16
F32 = jnp.float32
VMEM_LIMIT = 60 * 1024 * 1024
NT = (((1,), (1,)), ((), ()))
NN = (((1,), (0,)), ((), ()))


def dotf(a, b, dims):
    return lax.dot_general(a, b, dims, preferred_element_type=F32)


def rows8(x):
    return x.reshape(x.shape[0] // 8, 8, x.shape[1]) if x.ndim == 2 else x.reshape(x.shape[0] * 8, x.shape[2])


def all8(x):
    return jnp.broadcast_to(x, (8, x.shape[1]))


def params(**kw):
    return pltpu.CompilerParams(vmem_limit_bytes=VMEM_LIMIT, **kw)


def norm_kv_kernel(x_ref, g_ref, wk_ref, wv_ref, cos_ref, sin_ref, n_ref, *kv_refs):
    n_tok = x_ref.shape[1]
    half = n_tok // 2
    x = x_ref[0].astype(F32)
    inv = lax.rsqrt(jnp.mean(x * x, axis=-1, keepdims=True) + NORM_EPS)
    normed = rows8(rows8(x * inv) * g_ref[...]).astype(BF16)
    n_ref[...] = normed
    k_all = dotf(normed, wk_ref[...], NN)
    v_all = dotf(normed, wv_ref[...], NN)
    cos_t, sin_t = cos_ref[0], sin_ref[0]
    for h in range(wk_ref.shape[1] // HEAD_DIM):
        kv_ref, at = (kv_refs[0], 0) if h == 0 else (kv_refs[1], h - 1)
        cols = slice(h * HEAD_DIM, (h + 1) * HEAD_DIM)
        k = k_all[:, cols]
        k = (k * cos_t + pltpu.roll(k, HEAD_DIM // 2, 1) * sin_t).astype(BF16)
        v = v_all[:, cols].astype(BF16)
        for i in range(2):
            kv_ref[at, i, 0, :, :HEAD_DIM] = k[i * half:(i + 1) * half]
            kv_ref[at, i, 0, :, HEAD_DIM:] = v[i * half:(i + 1) * half]


def norm_kv(hidden, gain, w_k, w_v, cos_t, sin_t):
    n_batch, n_tok, d_model = hidden.shape
    kv_heads = w_k.shape[1] // HEAD_DIM
    half = n_tok // 2
    row = pl.BlockSpec((1, n_tok, HEAD_DIM), lambda i: (i, 0, 0))
    whole = pl.BlockSpec(w_k.shape, lambda i: (0, 0))
    parts = [1, kv_heads - 1] if kv_heads > 1 else [1]
    return pl.pallas_call(
        norm_kv_kernel,
        grid=(n_batch,),
        in_specs=[
            pl.BlockSpec((1, n_tok, d_model), lambda i: (i, 0, 0)),
            pl.BlockSpec((8, d_model), lambda i: (0, 0)),
            whole, whole, row, row,
        ],
        out_specs=[pl.BlockSpec((n_tok, d_model), lambda i: (i, 0))]
        + [pl.BlockSpec((n, 2, 1, half, 2 * HEAD_DIM), lambda i: (0, 0, i, 0, 0)) for n in parts],
        out_shape=[jax.ShapeDtypeStruct((n_batch * n_tok, d_model), BF16)]
        + [jax.ShapeDtypeStruct((n, 2, n_batch, half, 2 * HEAD_DIM), BF16) for n in parts],
        compiler_params=params(),
        cost_estimate=pl.CostEstimate(flops=4 * n_batch * n_tok * d_model * w_k.shape[1], bytes_accessed=4 * hidden.size + 4 * w_k.size, transcendentals=0),
        name="norm_kv",
    )(hidden, jnp.broadcast_to(gain.astype(F32), (8, d_model)), w_k, w_v, cos_t, sin_t)


def turn_kernel(i_ref, o_ref):
    o_ref[...] = i_ref[...].T


def turned(x, tile=256):
    n, m = x.shape
    return pl.pallas_call(
        turn_kernel,
        grid=(n // tile,),
        in_specs=[pl.BlockSpec((tile, m), lambda i: (i, 0))],
        out_specs=pl.BlockSpec((m, tile), lambda i: (0, i)),
        out_shape=jax.ShapeDtypeStruct((m, n), x.dtype),
        compiler_params=params(),
        cost_estimate=pl.CostEstimate(flops=400 * x.size, bytes_accessed=4 * x.size, transcendentals=0),
        name="turned",
    )(x)


def q_proj_kernel(n_ref, w_ref, cos_ref, sin_ref, q_ref):
    q = dotf(n_ref[...], w_ref[...], NN)
    cos_t, sin_t = cos_ref[...], sin_ref[...]
    for g in range(q.shape[1] // HEAD_DIM):
        cols = slice(g * HEAD_DIM, (g + 1) * HEAD_DIM)
        qg = q[:, cols]
        q_ref[:, cols] = (qg * cos_t + pltpu.roll(qg, HEAD_DIM // 2, 1) * sin_t).astype(BF16)


def q_proj(normed, w_q, cos_t, sin_t, h, width, tile=512):
    n_all, d_model = normed.shape
    return pl.pallas_call(
        q_proj_kernel,
        grid=(n_all // tile,),
        in_specs=[
            pl.BlockSpec((tile, d_model), lambda i: (i, 0)),
            pl.BlockSpec((d_model, width), lambda i: (0, h)),
            pl.BlockSpec((tile, HEAD_DIM), lambda i: (i, 0)),
            pl.BlockSpec((tile, HEAD_DIM), lambda i: (i, 0)),
        ],
        out_specs=pl.BlockSpec((tile, width), lambda i: (i, 0)),
        out_shape=jax.ShapeDtypeStruct((n_all, width), BF16),
        compiler_params=params(),
        cost_estimate=pl.CostEstimate(flops=2 * n_all * d_model * width, bytes_accessed=2 * n_all * d_model + 2 * d_model * width, transcendentals=0),
    )(normed, w_q, cos_t.reshape(n_all, HEAD_DIM), sin_t.reshape(n_all, HEAD_DIM))


def d_attn_kernel(dy_ref, w_ref, o_ref, da_ref, dl_ref):
    chunk = HEAD_DIM
    d_all = dotf(dy_ref[...], w_ref[...], NT).astype(BF16)
    da_ref[...] = d_all
    for g in range(d_all.shape[1] // HEAD_DIM):
        cols = slice(g * HEAD_DIM, (g + 1) * HEAD_DIM)
        prod = (d_all[:, cols].astype(F32) * o_ref[:, cols].astype(F32)).T
        total = all8(jnp.sum(prod, axis=0, keepdims=True))
        for i in range(total.shape[1] // chunk):
            dl_ref[i // 2, i % 2, :, cols] = total[:, i * chunk:(i + 1) * chunk]


def d_attn_of(dy, w_o, o_h, h, tile=512):
    n_all, d_model = dy.shape
    width = o_h.shape[1]
    rows = tile // (2 * HEAD_DIM)
    return pl.pallas_call(
        d_attn_kernel,
        grid=(n_all // tile,),
        in_specs=[
            pl.BlockSpec((tile, d_model), lambda i: (i, 0)),
            pl.BlockSpec((width, d_model), lambda i: (h, 0)),
            pl.BlockSpec((tile, width), lambda i: (i, 0)),
        ],
        out_specs=[
            pl.BlockSpec((tile, width), lambda i: (i, 0)),
            pl.BlockSpec((rows, 2, 8, width), lambda i: (i, 0, 0, 0)),
        ],
        out_shape=[
            jax.ShapeDtypeStruct((n_all, width), BF16),
            jax.ShapeDtypeStruct((n_all // (2 * HEAD_DIM), 2, 8, width), F32),
        ],
        compiler_params=params(),
        cost_estimate=pl.CostEstimate(flops=2 * n_all * d_model * width, bytes_accessed=2 * n_all * d_model + 2 * d_model * width, transcendentals=0),
    )(dy, w_o, o_h)


def pair_list(group):
    return [(2 * j, min(2, group - 2 * j)) for j in range((group + 1) // 2)]


def block_place(b, n_dev):
    half = (b >= n_dev // 2).astype(jnp.int32)
    dev = 2 * jnp.where(half == 1, n_dev - 1 - b, b)
    return dev, half


def block_mask(b, half, lo_row, hi_row):
    key = rows8(lax.broadcasted_iota(jnp.int32, (2 * HEAD_DIM, HEAD_DIM), 0))
    key = (key ^ (half * HEAD_DIM)) + b * (2 * HEAD_DIM)
    return (key >= lo_row) & (key <= hi_row)


def block_list(c, row, lo_sm, full_sm, qc_sm):
    lo, full, last = lo_sm[row, c], full_sm[row, c], qc_sm[c] // 2
    n_plain = last - full
    n_all = n_plain + full - lo + 1

    def block(t):
        m = lo + t - n_plain
        return jnp.where(t < n_plain, full + t, jnp.where(m < full, m, last))

    return n_plain, n_all, block


def run_blocks(blocks, first, step, even, odd):
    n_plain, n_all, block = blocks
    first(block(0))

    def pair(use_mask):
        def one(i, carry):
            t = 2 * i
            step(even, odd, block(t), block(t + 1), use_mask)
            step(odd, even, block(t + 1), block(t + 2), use_mask)
            return carry

        return one

    lax.fori_loop(0, n_plain // 2, pair(False), 0)
    lax.fori_loop(n_plain // 2, n_all // 2, pair(True), 0)

    @pl.when(n_all % 2 == 1)
    def _():
        step(even, None, block(n_all - 1), None, True)


def attn_fwd_kernel(lo_sm, full_sm, qc_sm, q_ref, kv_ref, lim_ref, o_ref, ot_ref, lse_ref, vt, qs, m_ref, l_ref, acc, s_a, s_b, *, group):
    row = pl.program_id(0)
    n_dev = kv_ref.shape[0]
    chunk = HEAD_DIM

    def key_block(b):
        dev, half = block_place(b, n_dev)
        return kv_ref.at[pl.ds(dev, 2), 0, half, 0]

    def turn(b, carry):
        v = key_block(b)[:, :, HEAD_DIM:].reshape(2 * chunk, HEAD_DIM)
        vt[b] = v.T
        return carry

    lax.fori_loop(jnp.minimum(lo_sm[row, 0], lo_sm[row, 1]), qc_sm[1] // 2 + 1, turn, 0)
    spans = [(slice(g0 * chunk, (g0 + ng) * chunk), ng) for g0, ng in pair_list(group)]
    n_span = len(spans)

    def one_chunk(c, carry):
        base = pl.multiple_of(c * chunk, chunk)
        for g in range(group):
            qs[g * chunk:(g + 1) * chunk, :] = q_ref[pl.ds(base, chunk), g * HEAD_DIM:(g + 1) * HEAD_DIM]
        m_ref[...] = jnp.full_like(m_ref, NEG_BIG)
        l_ref[...] = jnp.zeros_like(l_ref)
        acc[...] = jnp.zeros_like(acc)
        lo_row, hi_row = lim_ref[0, c, 0], lim_ref[0, c, 1]

        def keys_of(b):
            return key_block(b)[:, :, :HEAD_DIM].reshape(2 * chunk, HEAD_DIM)

        def step(now, later, b, b_next, use_mask):
            v_t = vt[b]

            def score(j):
                if later is not None and j < n_span:
                    cols = spans[j][0]
                    later[:, cols] = dotf(keys_of(b_next), qs[cols, :], NT)

            if use_mask:
                _, half = block_place(b, n_dev)
                ok = block_mask(b, half, lo_row, hi_row)
            score(0)
            for j, (cols, ng) in enumerate(spans):
                score(j + 1)
                s = rows8(now[:, cols])
                if use_mask:
                    s = jnp.concatenate([jnp.where(ok, s[:, :, i * chunk:(i + 1) * chunk], NEG_BIG) for i in range(ng)], axis=2)
                m_old = m_ref[:, cols]
                m_new = jnp.maximum(m_old, all8(jnp.max(jnp.max(s, axis=0), axis=0, keepdims=True)))
                p = jnp.exp2((s - m_new) * SCALE2)
                alpha = jnp.exp2((m_old - m_new) * SCALE2)
                m_ref[:, cols] = m_new
                l_ref[:, cols] = l_ref[:, cols] * alpha + jnp.sum(p, axis=0)
                acc[:, cols] = rows8(rows8(acc[:, cols]) * alpha) + dotf(v_t, rows8(p).astype(BF16), NN)

        def first(b):
            k = keys_of(b)
            for cols, _ in spans:
                s_a[:, cols] = dotf(k, qs[cols, :], NT)

        run_blocks(block_list(c, row, lo_sm, full_sm, qc_sm), first, step, s_a, s_b)
        l_all = all8(jnp.sum(l_ref[...], axis=0, keepdims=True))
        inv_l = 1.0 / l_all
        lse_ref[0, c] = m_ref[...] * SCALE2 + jnp.log(l_all) * LOG2E
        for g in range(group):
            cols = slice(g * chunk, (g + 1) * chunk)
            o_t = rows8(rows8(acc[:, cols]) * inv_l[:, cols])
            o_ref[pl.ds(base, chunk), cols] = o_t.T.astype(BF16)
            ot_ref[cols, pl.ds(base, chunk)] = o_t.astype(BF16)
        return carry

    lax.fori_loop(0, 2, one_chunk, 0)


def attn_cost(n_rows, n_dev, width, n_mat):
    pairs = n_rows * (2 * n_dev + 1) * 128 * 128 * (width // HEAD_DIM)
    return pl.CostEstimate(flops=4 * n_mat * pairs * HEAD_DIM, bytes_accessed=8 * n_rows * 256 * width, transcendentals=pairs)


def attn_fwd(scalars, q, kv, at, limits):
    n_all, width = q.shape
    n_dev, _, _, n_rows, chunk, _ = kv.shape
    group = width // HEAD_DIM
    n_tok = n_all // n_rows
    return pl.pallas_call(
        functools.partial(attn_fwd_kernel, group=group),
        grid_spec=pltpu.PrefetchScalarGridSpec(
            num_scalar_prefetch=3,
            grid=(n_rows,),
            in_specs=[
                pl.BlockSpec((n_tok, width), lambda i, *_: (i, 0)),
                pl.BlockSpec((n_dev, 1, 2, 1, chunk, 2 * HEAD_DIM), lambda i, *_: (0, at, 0, i, 0, 0)),
                pl.BlockSpec((1, 2, 2, 8, chunk), lambda i, *_: (i, 0, 0, 0, 0)),
            ],
            out_specs=[
                pl.BlockSpec((n_tok, width), lambda i, *_: (i, 0)),
                pl.BlockSpec((width, n_tok), lambda i, *_: (0, i)),
                pl.BlockSpec((1, 2, 8, width), lambda i, *_: (i, 0, 0, 0)),
            ],
            scratch_shapes=[
                pltpu.VMEM((n_dev, HEAD_DIM, 2 * chunk), BF16),
                pltpu.VMEM((group * chunk, HEAD_DIM), BF16),
                pltpu.VMEM((8, width), F32),
                pltpu.VMEM((8, width), F32),
                pltpu.VMEM((HEAD_DIM, width), F32),
                pltpu.VMEM((2 * chunk, width), F32),
                pltpu.VMEM((2 * chunk, width), F32),
            ],
        ),
        out_shape=[
            jax.ShapeDtypeStruct((n_all, width), BF16),
            jax.ShapeDtypeStruct((width, n_all), BF16),
            jax.ShapeDtypeStruct((n_rows, 2, 8, width), F32),
        ],
        compiler_params=params(),
        cost_estimate=attn_cost(n_rows, n_dev, width, 2),
    )(*scalars, q, kv, limits)


def attn_bwd_kernel(lo_sm, full_sm, qc_sm, q_ref, kv_ref, lim_ref, do_ref, lse_ref, dl_ref, cos_ref, sin_ref, dq_ref, keep_ref, send_ref, kt, qs, dos, dqt, dkv_ref, s_a, s_b, d_a, d_b, *, group):
    row = pl.program_id(0)
    n_dev = kv_ref.shape[0]
    chunk = HEAD_DIM
    dkv_ref[...] = jnp.zeros_like(dkv_ref)

    def key_block(b):
        dev, half = block_place(b, n_dev)
        return kv_ref.at[pl.ds(dev, 2), 0, half, 0]

    def turn(b, carry):
        k = key_block(b)[:, :, :HEAD_DIM].reshape(2 * chunk, HEAD_DIM)
        kt[b] = k.T
        return carry

    lax.fori_loop(jnp.minimum(lo_sm[row, 0], lo_sm[row, 1]), qc_sm[1] // 2 + 1, turn, 0)
    spans = [(slice(g0 * chunk, (g0 + ng) * chunk), ng) for g0, ng in pair_list(group)]

    def one_chunk(c, carry):
        base = pl.multiple_of(c * chunk, chunk)
        for g in range(group):
            cols = slice(g * HEAD_DIM, (g + 1) * HEAD_DIM)
            qs[g * chunk:(g + 1) * chunk, :] = q_ref[pl.ds(base, chunk), cols]
            dos[g * chunk:(g + 1) * chunk, :] = do_ref[pl.ds(base, chunk), cols]
        dqt[...] = jnp.zeros_like(dqt)
        lo_row, hi_row = lim_ref[0, c, 0], lim_ref[0, c, 1]

        def keys_of(b):
            kv = key_block(b)[...].reshape(2 * chunk, 2 * HEAD_DIM)
            return kv[:, :HEAD_DIM], kv[:, HEAD_DIM:]

        def score(later, k, v, j):
            cols = spans[j][0]
            later[0][:, cols] = dotf(k, qs[cols, :], NT)
            later[1][:, cols] = dotf(v, dos[cols, :], NT)

        def step(now, later, b, b_next, use_mask):
            dev, half = block_place(b, n_dev)
            k_t = kt[b]
            if use_mask:
                ok = block_mask(b, half, lo_row, hi_row)
            dk = jnp.zeros((2 * chunk, HEAD_DIM), F32)
            dv = jnp.zeros((2 * chunk, HEAD_DIM), F32)

            def ahead(j):
                if later is not None and j < len(spans):
                    score(later, *keys_of(b_next), j)

            ahead(0)
            for j, (cols, ng) in enumerate(spans):
                ahead(j + 1)
                p = jnp.exp2(rows8(now[0][:, cols]) * SCALE2 - lse_ref[0, c, :, cols])
                if use_mask:
                    p = jnp.concatenate([jnp.where(ok, p[:, :, i * chunk:(i + 1) * chunk], 0.0) for i in range(ng)], axis=2)
                ds = rows8(p * (rows8(now[1][:, cols]) - dl_ref[0, c, :, cols])).astype(BF16)
                dv = dv + dotf(rows8(p).astype(BF16), dos[cols, :], NN)
                dk = dk + dotf(ds, qs[cols, :], NN)
                dqt[:, cols] += dotf(k_t, ds, NN)
            out = dkv_ref.at[pl.ds(dev, 2), half]
            out[:, :, :HEAD_DIM] += (dk * SCALE).reshape(2, chunk, HEAD_DIM)
            out[:, :, HEAD_DIM:] += dv.reshape(2, chunk, HEAD_DIM)

        def first(b):
            for j in range(len(spans)):
                score((s_a, d_a), *keys_of(b), j)

        run_blocks(block_list(c, row, lo_sm, full_sm, qc_sm), first, step, (s_a, d_a), (s_b, d_b))
        cos_t, sin_t = cos_ref[0, c], sin_ref[0, c]
        for g in range(group):
            cols = slice(g * chunk, (g + 1) * chunk)
            d = dqt[:, cols] * SCALE
            a, b = d[:HEAD_DIM // 2], d[HEAD_DIM // 2:]
            turned = jnp.concatenate([a * cos_t + b * sin_t, b * cos_t - a * sin_t], axis=0)
            dq_ref[pl.ds(base, chunk), cols] = turned.T.astype(BF16)
        return carry

    lax.fori_loop(0, 2, one_chunk, 0)
    core = qc_sm[2]
    for i in range(n_dev // 2):
        for half in range(2):
            keep_ref[i, half, 0] = dkv_ref[2 * i + core, half]
            send_ref[i, half, 0] = dkv_ref[2 * i + 1 - core, half]


def attn_bwd(scalars, q, kv, at, limits, d_o, lse, delta, cos_c, sin_c):
    n_all, width = q.shape
    n_dev, _, _, n_rows, chunk, _ = kv.shape
    group = width // HEAD_DIM
    n_tok = n_all // n_rows
    tok = pl.BlockSpec((n_tok, width), lambda i, *_: (i, 0))
    kvs = pl.BlockSpec((n_dev, 1, 2, 1, chunk, 2 * HEAD_DIM), lambda i, *_: (0, at, 0, i, 0, 0))
    dkvs = pl.BlockSpec((n_dev // 2, 2, 1, chunk, 2 * HEAD_DIM), lambda i, *_: (0, 0, i, 0, 0))
    stat = pl.BlockSpec((1, 2, 8, width), lambda i, *_: (i, 0, 0, 0))
    rope = pl.BlockSpec((1, 2, HEAD_DIM // 2, chunk), lambda i, *_: (i, 0, 0, 0))
    return pl.pallas_call(
        functools.partial(attn_bwd_kernel, group=group),
        grid_spec=pltpu.PrefetchScalarGridSpec(
            num_scalar_prefetch=3,
            grid=(n_rows,),
            in_specs=[tok, kvs, pl.BlockSpec((1, 2, 2, 8, chunk), lambda i, *_: (i, 0, 0, 0, 0)), tok, stat, stat, rope, rope],
            out_specs=[tok, dkvs, dkvs],
            scratch_shapes=[
                pltpu.VMEM((n_dev, HEAD_DIM, 2 * chunk), BF16),
                pltpu.VMEM((group * chunk, HEAD_DIM), BF16),
                pltpu.VMEM((group * chunk, HEAD_DIM), BF16),
                pltpu.VMEM((HEAD_DIM, width), F32),
                pltpu.VMEM((n_dev, 2, chunk, 2 * HEAD_DIM), F32),
            ] + [pltpu.VMEM((2 * chunk, width), F32)] * 4,
        ),
        out_shape=[jax.ShapeDtypeStruct((n_all, width), BF16)]
        + [jax.ShapeDtypeStruct((n_dev // 2, 2, n_rows, chunk, 2 * HEAD_DIM), F32)] * 2,
        compiler_params=params(),
        cost_estimate=attn_cost(n_rows, n_dev, width, 5),
    )(*scalars, q, kv, limits, d_o, lse, delta, cos_c, sin_c)


def grid_spec(n_prefetch, grid, in_specs, out_specs):
    return pltpu.PrefetchScalarGridSpec(num_scalar_prefetch=n_prefetch, grid=grid, in_specs=in_specs, out_specs=out_specs)


def both_tokens(own_ref, pair_ref, rhs_ref, rhs_pair_ref):
    return dotf(own_ref[...], rhs_ref[...], NN) + dotf(pair_ref[...], rhs_pair_ref[...], NN)


def grad_parts_kernel(order_sm, own_ref, pair_ref, rhs_ref, rhs_pair_ref, sx_ref, sy_ref, k_ref):
    i = pl.program_id(0)
    part = both_tokens(own_ref, pair_ref, rhs_ref, rhs_pair_ref)

    @pl.when(i < 2)
    def _():
        sx_ref[0] = part

    @pl.when((i >= 2) & (i < 4))
    def _():
        sy_ref[0] = part

    @pl.when(i >= 4)
    def _():
        k_ref[0] = part


def grad_specs(rhs, tile, own_at, pair_at):
    n_all, cols = rhs.shape
    whole = pl.BlockSpec((n_all, cols), lambda i, *_: (0, 0), pipeline_mode=pl.Buffered(1))
    cost = pl.CostEstimate(flops=4 * 8 * tile * n_all * cols, bytes_accessed=4 * n_all * (8 * tile + cols) + 32 * tile * cols, transcendentals=0)
    return [pl.BlockSpec((tile, n_all), own_at), pl.BlockSpec((tile, n_all), pair_at), whole, whole], cost


def grad_parts(order, own, pair, rhs, rhs_pair):
    tile, cols = pair.shape[0] // 8, rhs.shape[1]
    own_base = lambda order: order[8] if own.shape[0] > pair.shape[0] else 0
    in_specs, cost = grad_specs(rhs, tile, lambda i, order: (order[i] + own_base(order), 0), lambda i, order: (order[i], 0))
    block = (1, tile, cols)
    return pl.pallas_call(
        grad_parts_kernel,
        grid_spec=grid_spec(1, (8,), in_specs, [
            pl.BlockSpec(block, lambda i, order: (jnp.minimum(i, 1), 0, 0)),
            pl.BlockSpec(block, lambda i, order: (jnp.clip(i - 2, 0, 1), 0, 0)),
            pl.BlockSpec(block, lambda i, order: (jnp.maximum(i - 4, 0), 0, 0))]),
        out_shape=[jax.ShapeDtypeStruct((n, tile, cols), F32) for n in (2, 2, 4)],
        compiler_params=params(),
        cost_estimate=cost,
    )(order, own, pair, rhs, rhs_pair)


def grad_whole_kernel(order_sm, own_ref, pair_ref, rhs_ref, rhs_pair_ref, o_ref):
    o_ref[...] = both_tokens(own_ref, pair_ref, rhs_ref, rhs_pair_ref)


def grad_whole(order, own, pair, rhs, rhs_pair):
    tile, cols = pair.shape[0] // 8, rhs.shape[1]
    in_specs, cost = grad_specs(rhs, tile, lambda i, order: (i + order[8], 0), lambda i, order: (i, 0))
    return pl.pallas_call(
        grad_whole_kernel,
        grid_spec=grid_spec(1, (8,), in_specs, [pl.BlockSpec((tile, cols), lambda i, order: (i, 0))]),
        out_shape=[jax.ShapeDtypeStruct((8 * tile, cols), F32)],
        compiler_params=params(),
        cost_estimate=cost,
    )(order, own, pair, rhs, rhs_pair)[0]


def add_parts_kernel(at_sm, a_ref, b_ref, c_ref, d_ref, ra_ref, rb_ref, rc_ref, rd_ref, *o_refs):
    for o_ref, k_ref, r_ref in zip(o_refs, (a_ref, b_ref, c_ref, d_ref), (ra_ref, rb_ref, rc_ref, rd_ref)):
        o_ref[...] = k_ref[0] + r_ref[0]


def add_parts(at, kept, rx, ry):
    _, rows, cols = kept.shape
    n = 2
    block = (1, rows // n, cols)
    part = lambda j: pl.BlockSpec(block, lambda i, at: (j, i, 0))
    recv = lambda f: pl.BlockSpec(block, lambda i, at: (f(at[0], at[1]), i, 0))
    out = pl.BlockSpec((rows // n, cols), lambda i, at: (i, 0))
    return pl.pallas_call(
        add_parts_kernel,
        grid_spec=grid_spec(1, (n,), [part(j) for j in range(4)] + [
            recv(lambda x, y: y), recv(lambda x, y: 1 - y), recv(lambda x, y: x), recv(lambda x, y: 1 - x)], [out] * 4),
        out_shape=[jax.ShapeDtypeStruct((rows, cols), F32)] * 4,
        compiler_params=params(),
        cost_estimate=pl.CostEstimate(flops=2 * kept.size, bytes_accessed=12 * kept.size, transcendentals=0),
        name="add_parts",
    )(at, *([kept] * 4), rx, rx, ry, ry)


def add_last_kernel(a_ref, ra_ref, b_ref, rb_ref, o_ref):
    o_ref[0] = a_ref[...] + ra_ref[...]
    o_ref[1] = b_ref[...] + rb_ref[...]


def add_last(k1, r1, k2, r2):
    rows, cols = k1.shape
    n = 2
    one = pl.BlockSpec((rows // n, cols), lambda i: (i, 0))
    return pl.pallas_call(
        add_last_kernel,
        grid=(n,),
        in_specs=[one] * 4,
        out_specs=pl.BlockSpec((2, rows // n, cols), lambda i: (0, i, 0)),
        out_shape=jax.ShapeDtypeStruct((2, rows, cols), F32),
        compiler_params=params(),
        cost_estimate=pl.CostEstimate(flops=2 * k1.size, bytes_accessed=24 * k1.size, transcendentals=0),
        name="add_last",
    )(k1, r1, k2, r2)


def sum_core_kernel(at_sm, keep_ref, got_ref, kx_ref, sx_ref, ky_ref, sy_ref):
    x, y = at_sm[0], at_sm[1]
    for i in range(2):
        for o_ref, j in ((kx_ref, x), (sx_ref, 1 - x)):
            o_ref[i, 0] = keep_ref[i, j, 0, 0] + got_ref[i, j, 0, 0]
        for o_ref, j in ((ky_ref, y), (sy_ref, 1 - y)):
            o_ref[i, 0] = keep_ref[j, i, 1, 0] + got_ref[j, i, 1, 0]


def sum_core(at, keep, got):
    shape = keep.shape[3:]
    cells = pl.BlockSpec((2, 2, 2, 1) + shape[1:], lambda i, *_: (0, 0, 0, i, 0, 0))
    pair = pl.BlockSpec((2, 1) + shape[1:], lambda i, *_: (0, i, 0, 0))
    return pl.pallas_call(
        sum_core_kernel,
        grid_spec=pltpu.PrefetchScalarGridSpec(num_scalar_prefetch=1, grid=(shape[0],), in_specs=[cells] * 2, out_specs=[pair] * 4),
        out_shape=[jax.ShapeDtypeStruct((2,) + shape, F32)] * 4,
        compiler_params=params(),
        cost_estimate=pl.CostEstimate(flops=8 * keep.size, bytes_accessed=12 * keep.size, transcendentals=0),
        name="sum_core",
    )(at, keep, got)


def sum_axis_kernel(at_sm, kx_ref, rx_ref, ky_ref, ry_ref, k1_ref, s1_ref, k2_ref, s2_ref):
    x, y = at_sm[0], at_sm[1]
    for o_ref, j in ((k1_ref, y), (s1_ref, 1 - y)):
        o_ref[0] = kx_ref[j, 0] + rx_ref[j, 0]
    for o_ref, j in ((k2_ref, x), (s2_ref, 1 - x)):
        o_ref[0] = ky_ref[j, 0] + ry_ref[j, 0]


def sum_axis(at, kx, rx, ky, ry):
    shape = kx.shape[1:]
    pair = pl.BlockSpec((2, 1) + shape[1:], lambda i, *_: (0, i, 0, 0))
    one = pl.BlockSpec((1,) + shape[1:], lambda i, *_: (i, 0, 0))
    return pl.pallas_call(
        sum_axis_kernel,
        grid_spec=pltpu.PrefetchScalarGridSpec(num_scalar_prefetch=1, grid=(shape[0],), in_specs=[pair] * 4, out_specs=[one] * 4),
        out_shape=[jax.ShapeDtypeStruct(shape, F32)] * 4,
        compiler_params=params(),
        cost_estimate=pl.CostEstimate(flops=8 * kx.size, bytes_accessed=24 * kx.size, transcendentals=0),
        name="sum_axis",
    )(at, kx, rx, ky, ry)


def sum_last_kernel(cos_ref, sin_ref, *refs):
    *in_refs, o_ref = refs
    chunk = HEAD_DIM
    for h in range(len(in_refs) // 4):
        for half in range(2):
            a_ref, b_ref = in_refs[4 * h + 2 * half], in_refs[4 * h + 2 * half + 1]
            rows = slice(half * chunk, (half + 1) * chunk)
            total = a_ref[0] + b_ref[0]
            dk = total[:, :HEAD_DIM]
            dk = dk * cos_ref[0, rows] - pltpu.roll(dk, HEAD_DIM // 2, 1) * sin_ref[0, rows]
            at_k, at_v = h * HEAD_DIM, o_ref.shape[1] // 2 + h * HEAD_DIM
            o_ref[rows, at_k:at_k + HEAD_DIM] = dk.astype(BF16)
            o_ref[rows, at_v:at_v + HEAD_DIM] = total[:, HEAD_DIM:].astype(BF16)


def sum_last(cos_t, sin_t, parts):
    n_rows, n_tok, _ = cos_t.shape
    shape = parts[0].shape
    rope = pl.BlockSpec((1, n_tok, HEAD_DIM), lambda i: (i, 0, 0))
    one = pl.BlockSpec((1,) + shape[1:], lambda i: (i, 0, 0))
    cols = len(parts) // 4 * shape[2]
    return pl.pallas_call(
        sum_last_kernel,
        grid=(n_rows,),
        in_specs=[rope] * 2 + [one] * len(parts),
        out_specs=pl.BlockSpec((n_tok, cols), lambda i: (i, 0)),
        out_shape=jax.ShapeDtypeStruct((n_rows * n_tok, cols), BF16),
        compiler_params=params(),
        cost_estimate=pl.CostEstimate(flops=8 * parts[0].size * len(parts), bytes_accessed=4 * parts[0].size * len(parts), transcendentals=0),
        name="sum_last",
    )(cos_t, sin_t, *parts)


def copy_kernel(i_ref, *refs):
    o_ref = refs[-1]
    o_ref[...] = i_ref[...].reshape(o_ref.shape)


def split_kernel(i_ref, k_ref, v_ref):
    k_ref[...] = i_ref[0, :, :k_ref.shape[1]]
    v_ref[...] = i_ref[0, :, k_ref.shape[1]:]


def place(x, grid, in_spec, outs, kernel=copy_kernel, into=None):
    return pl.pallas_call(
        kernel,
        grid=grid,
        in_specs=[in_spec] + [pl.BlockSpec(memory_space=pl.ANY)] * (into is not None),
        out_specs=[spec for _, spec in outs],
        out_shape=[jax.ShapeDtypeStruct(shape, x.dtype) for shape, _ in outs],
        input_output_aliases={} if into is None else {1: 0},
        compiler_params=params(),
        cost_estimate=pl.CostEstimate(flops=x.size, bytes_accessed=8 * x.size, transcendentals=0),
    )(*([x] if into is None else [x, into]))


def solution(mesh):
    n_dev = mesh.shape['cp']

    def block(hidden, grad_out, positions, seg_ids, w_q, w_k, w_v, w_o, norm_gain):
        n_batch, n_tok, d_model = hidden.shape
        n_all = n_batch * n_tok
        chunk = n_tok // 2
        kv_heads = w_k.shape[1] // HEAD_DIM
        width = w_q.shape[1] // kv_heads
        heads = range(kv_heads)
        rank = lax.axis_index('cp')

        q_chunks = jnp.stack([rank, 2 * n_dev - 1 - rank, rank & 1]).astype(jnp.int32)
        glob = (q_chunks[:2, None] * chunk + jnp.arange(chunk, dtype=jnp.int32)[None, :])
        pos_c = positions.reshape(n_batch, 2, chunk)
        doc_start = glob[None] - pos_c
        limits = jnp.stack([doc_start, jnp.broadcast_to(glob[None], doc_start.shape)], axis=2)
        limits = jnp.broadcast_to(limits[:, :, :, None], (n_batch, 2, 2, 8, chunk))
        blk = 2 * chunk
        last = q_chunks[:2] // 2
        lo_blk = doc_start[:, :, 0] // blk
        full_blk = jnp.minimum((doc_start[:, :, -1] + blk - 1) // blk, last[None, :])
        scalars = (lo_blk, full_blk, q_chunks)

        inv_freq = ROPE_BASE ** (-jnp.arange(0, HEAD_DIM, 2).astype(F32) / HEAD_DIM)
        pos_f = positions.astype(F32)
        ang = pos_f[..., None] * inv_freq
        cos_h, sin_h = jnp.cos(ang), jnp.sin(ang)
        cos_t = jnp.concatenate([cos_h, cos_h], axis=-1)
        sin_t = jnp.concatenate([-sin_h, sin_h], axis=-1)
        cos_c = jnp.swapaxes(cos_h.reshape(n_batch, 2, chunk, HEAD_DIM // 2), 2, 3)
        sin_c = jnp.swapaxes(sin_h.reshape(n_batch, 2, chunk, HEAD_DIM // 2), 2, 3)

        cos_t, sin_t = lax.optimization_barrier((cos_t, sin_t))
        core, at = rank & 1, jnp.stack([(rank >> 1) & 1, (rank >> 2) & 1]).astype(jnp.int32)

        def send(value, bit):
            return lax.ppermute(value, 'cp', [(i, i ^ bit) for i in range(n_dev)])

        x_at, y_at = at[0], at[1]
        cell = lambda y, x, half: (y * 2 + x) * 2 + half
        order = jnp.stack(
            [cell(0, 1 - x_at, 0), cell(1, 1 - x_at, 0), cell(1 - y_at, 0, 1), cell(1 - y_at, 1, 1)]
            + [cell(y_at, x_at, 0), cell(1 - y_at, x_at, 0), cell(y_at, x_at, 1), cell(y_at, 1 - x_at, 1), 8 * core]).astype(jnp.int32)

        def share(own, pair, rhs, rhs_pair):
            sx, sy, kept = grad_parts(order, own, pair, rhs, rhs_pair)
            rx, ry = send(sx, 2), send(sy, 4)
            k1, s1, k2, s2 = add_parts(at, kept, rx, ry)
            r1, r2 = send(s1, 4), send(s2, 2)
            total = add_last(k1, r1, k2, r2)
            return total.reshape(-1, total.shape[-1])

        def half_cols(value, which):
            return lax.dynamic_slice_in_dim(value, which * (d_model // 2), d_model // 2, 1)

        same_core = [[i + j for i in range(0, n_dev, 2)] for j in range(2)]
        scatter = functools.partial(lax.psum_scatter, axis_name='cp', scatter_dimension=0, axis_index_groups=same_core, tiled=True)
        gather = functools.partial(lax.all_gather, axis_name='cp', axis=0, tiled=False)

        normed, *kv_loc = norm_kv(hidden, norm_gain, w_k, w_v, cos_t, sin_t)
        kv_parts = []
        for part in kv_loc:
            kv_parts.append(gather(part))
        kv_of = [(kv_parts[0], 0)] + [(kv_parts[-1], h - 1) for h in heads[1:]]

        dy = grad_out.reshape(n_all, d_model)
        dy_own, dy_pair = half_cols(dy, core), send(half_cols(dy, 1 - core), 1)
        n_t = turned(normed)
        n_pair = send(lax.dynamic_slice_in_dim(n_t, (1 - core) * (d_model // 2), d_model // 2, 0), 1)
        q, attn, lse, gwo, d_attn, delta = [], [], [], [], [], []
        for h in heads:
            q.append(q_proj(normed, w_q, cos_t, sin_t, h, width))
            o_h, ot_h, lse_h = attn_fwd(scalars, q[h], *kv_of[h], limits)
            attn.append(o_h)
            lse.append(lse_h)
            own = share(ot_h, send(ot_h, 1), dy_own, dy_pair)
            gwo.append(gather(own))
            d_attn_h, delta_h = d_attn_of(dy, w_o, o_h, h)
            d_attn.append(d_attn_h)
            delta.append(delta_h)

        dq, dkv, gwq = [], [], []
        for h in heads:
            dq_h, keep, give = attn_bwd(scalars, q[h], *kv_of[h], limits, d_attn[h], lse[h], delta[h], cos_c, sin_c)
            dq.append(dq_h)
            own = share(n_t, n_pair, dq_h, send(dq_h, 1))
            gwq.append(gather(own))
            got = send(give, 1)
            cells = (2, 2) + keep.shape[1:]
            kx, sx, ky, sy = sum_core(at, keep.reshape(cells), got.reshape(cells))
            rx, ry = send(sx, 2), send(sy, 4)
            k1, s1, k2, s2 = sum_axis(at, kx, rx, ky, ry)
            dkv += [k1, send(s1, 4), k2, send(s2, 2)]

        attn_flat = jnp.concatenate(attn, axis=1)
        proj_out = dotf(attn_flat, w_o, NN).reshape(hidden.shape)
        block_out = (hidden.astype(F32) + proj_out).astype(BF16)
        dq_flat = jnp.concatenate(dq, axis=1)
        d_norm_q = dotf(dq_flat, w_q, NT)

        dkv_lin = sum_last(cos_t, sin_t, dkv)
        dkv_pair = send(dkv_lin, 1)
        part = grad_whole(order, n_t, n_pair, dkv_lin, dkv_pair)
        gwkv = scatter(part)

        w_kv = jnp.concatenate([w_k, w_v], axis=1)
        d_norm_kv = dotf(dkv_lin, w_kv, NT)
        d_normed = (d_norm_q + d_norm_kv).astype(BF16).astype(F32)
        x = hidden.astype(F32).reshape(n_all, d_model)
        inv = lax.rsqrt(jnp.mean(x * x, axis=-1, keepdims=True) + NORM_EPS)
        xn = x * inv
        u = d_normed * norm_gain.astype(F32)
        d_x = inv * (u - xn * jnp.mean(u * xn, axis=-1, keepdims=True))
        grad_hidden = (dy.astype(F32) + d_x).astype(BF16).reshape(hidden.shape)
        grad_gain = jnp.sum(d_normed * xn, axis=0)
        for bit in (1, 2, 4):
            grad_gain = grad_gain + send(grad_gain, bit)
        gwkv_all = gather(gwkv)

        n_chip = n_dev // 2
        rows_o, rows_q = width // n_chip, d_model // n_dev
        grad_wo = grad_wq = None
        for h in heads:
            grad_wo, = place(
                gwo[h], (n_dev,), pl.BlockSpec((1, rows_o, d_model // 2), lambda d: (d, 0, 0)),
                [(w_o.shape, pl.BlockSpec((rows_o, d_model // 2), lambda d, h=h: (h * n_chip + d // 2, d % 2)))], into=grad_wo)
        at_q = lambda d: ((d % 2) * n_chip + d // 2, 0)
        for h in heads:
            grad_wq, = place(
                gwq[h], (n_dev,), pl.BlockSpec((1, rows_q, width), lambda d: (d, 0, 0)),
                [(w_q.shape, pl.BlockSpec((rows_q, width), lambda d, h=h: (at_q(d)[0], h)))], into=grad_wq)
        grad_wk, grad_wv = place(
            gwkv_all, (n_dev,), pl.BlockSpec((1, rows_q, 2 * w_k.shape[1]), lambda d: (d, 0, 0)),
            [(w_k.shape, pl.BlockSpec((rows_q, w_k.shape[1]), at_q))] * 2, split_kernel)
        return block_out, grad_hidden, grad_wq, grad_wk, grad_wv, grad_wo, grad_gain

    seq_spec = P(None, 'cp', None)
    tok_spec = P(None, 'cp')
    full = P()
    return jax.shard_map(block, mesh=mesh, in_specs=(seq_spec, seq_spec, tok_spec, tok_spec, full, full, full, full, full), out_specs=(seq_spec, seq_spec, full, full, full, full, full), check_vma=False)
```

```python
import functools
import math

import jax
import jax.numpy as jnp
from jax import lax
from jax.experimental import pallas as pl
from jax.experimental.pallas import tpu as pltpu
from jax.sharding import PartitionSpec as P


HEAD_DIM = 128
NORM_EPS = 1e-5
ROPE_BASE = 500000.0
NEG_BIG = -1e30
SCALE = HEAD_DIM ** -0.5
LOG2E = math.log2(math.e)
SCALE2 = SCALE * LOG2E
BF16 = jnp.bfloat16
F32 = jnp.float32
VMEM_LIMIT = 60 * 1024 * 1024
NT = (((1,), (1,)), ((), ()))
NN = (((1,), (0,)), ((), ()))


def dotf(a, b, dims):
    return lax.dot_general(a, b, dims, preferred_element_type=F32)


def rows8(x):
    return x.reshape(x.shape[0] // 8, 8, x.shape[1]) if x.ndim == 2 else x.reshape(x.shape[0] * 8, x.shape[2])


def all8(x):
    return jnp.broadcast_to(x, (8, x.shape[1]))


def params(**kw):
    return pltpu.CompilerParams(vmem_limit_bytes=VMEM_LIMIT, **kw)


def norm_kv_kernel(x_ref, g_ref, wk_ref, wv_ref, cos_ref, sin_ref, n_ref, *kv_refs):
    n_tok = x_ref.shape[1]
    half = n_tok // 2
    x = x_ref[0].astype(F32)
    inv = lax.rsqrt(jnp.mean(x * x, axis=-1, keepdims=True) + NORM_EPS)
    normed = rows8(rows8(x * inv) * g_ref[...]).astype(BF16)
    n_ref[...] = normed
    k_all = dotf(normed, wk_ref[...], NN)
    v_all = dotf(normed, wv_ref[...], NN)
    cos_t, sin_t = cos_ref[0], sin_ref[0]
    for h in range(wk_ref.shape[1] // HEAD_DIM):
        kv_ref, at = (kv_refs[0], 0) if h == 0 else (kv_refs[1], h - 1)
        cols = slice(h * HEAD_DIM, (h + 1) * HEAD_DIM)
        k = k_all[:, cols]
        k = (k * cos_t + pltpu.roll(k, HEAD_DIM // 2, 1) * sin_t).astype(BF16)
        v = v_all[:, cols].astype(BF16)
        for i in range(2):
            kv_ref[at, i, 0, :, :HEAD_DIM] = k[i * half:(i + 1) * half]
            kv_ref[at, i, 0, :, HEAD_DIM:] = v[i * half:(i + 1) * half]


def norm_kv(hidden, gain, w_k, w_v, cos_t, sin_t):
    n_batch, n_tok, d_model = hidden.shape
    kv_heads = w_k.shape[1] // HEAD_DIM
    half = n_tok // 2
    row = pl.BlockSpec((1, n_tok, HEAD_DIM), lambda i: (i, 0, 0))
    whole = pl.BlockSpec(w_k.shape, lambda i: (0, 0))
    parts = [1, kv_heads - 1] if kv_heads > 1 else [1]
    return pl.pallas_call(
        norm_kv_kernel,
        grid=(n_batch,),
        in_specs=[
            pl.BlockSpec((1, n_tok, d_model), lambda i: (i, 0, 0)),
            pl.BlockSpec((8, d_model), lambda i: (0, 0)),
            whole, whole, row, row,
        ],
        out_specs=[pl.BlockSpec((n_tok, d_model), lambda i: (i, 0))]
        + [pl.BlockSpec((n, 2, 1, half, 2 * HEAD_DIM), lambda i: (0, 0, i, 0, 0)) for n in parts],
        out_shape=[jax.ShapeDtypeStruct((n_batch * n_tok, d_model), BF16)]
        + [jax.ShapeDtypeStruct((n, 2, n_batch, half, 2 * HEAD_DIM), BF16) for n in parts],
        compiler_params=params(),
        cost_estimate=pl.CostEstimate(flops=4 * n_batch * n_tok * d_model * w_k.shape[1], bytes_accessed=4 * hidden.size + 4 * w_k.size, transcendentals=0),
        name="norm_kv",
    )(hidden, jnp.broadcast_to(gain.astype(F32), (8, d_model)), w_k, w_v, cos_t, sin_t)


def turn_kernel(i_ref, o_ref):
    o_ref[...] = i_ref[...].T


def turned(x, tile=256):
    n, m = x.shape
    return pl.pallas_call(
        turn_kernel,
        grid=(n // tile,),
        in_specs=[pl.BlockSpec((tile, m), lambda i: (i, 0))],
        out_specs=pl.BlockSpec((m, tile), lambda i: (0, i)),
        out_shape=jax.ShapeDtypeStruct((m, n), x.dtype),
        compiler_params=params(),
        cost_estimate=pl.CostEstimate(flops=400 * x.size, bytes_accessed=4 * x.size, transcendentals=0),
        name="turned",
    )(x)


def q_proj_kernel(n_ref, w_ref, cos_ref, sin_ref, q_ref):
    q = dotf(n_ref[...], w_ref[...], NN)
    cos_t, sin_t = cos_ref[...], sin_ref[...]
    for g in range(q.shape[1] // HEAD_DIM):
        cols = slice(g * HEAD_DIM, (g + 1) * HEAD_DIM)
        qg = q[:, cols]
        q_ref[:, cols] = (qg * cos_t + pltpu.roll(qg, HEAD_DIM // 2, 1) * sin_t).astype(BF16)


def q_proj(normed, w_q, cos_t, sin_t, h, width, tile=512):
    n_all, d_model = normed.shape
    return pl.pallas_call(
        q_proj_kernel,
        grid=(n_all // tile,),
        in_specs=[
            pl.BlockSpec((tile, d_model), lambda i: (i, 0)),
            pl.BlockSpec((d_model, width), lambda i: (0, h)),
            pl.BlockSpec((tile, HEAD_DIM), lambda i: (i, 0)),
            pl.BlockSpec((tile, HEAD_DIM), lambda i: (i, 0)),
        ],
        out_specs=pl.BlockSpec((tile, width), lambda i: (i, 0)),
        out_shape=jax.ShapeDtypeStruct((n_all, width), BF16),
        compiler_params=params(),
        cost_estimate=pl.CostEstimate(flops=2 * n_all * d_model * width, bytes_accessed=2 * n_all * d_model + 2 * d_model * width, transcendentals=0),
    )(normed, w_q, cos_t.reshape(n_all, HEAD_DIM), sin_t.reshape(n_all, HEAD_DIM))


def d_attn_kernel(dy_ref, w_ref, o_ref, da_ref, dl_ref):
    chunk = HEAD_DIM
    d_all = dotf(dy_ref[...], w_ref[...], NT).astype(BF16)
    da_ref[...] = d_all
    for g in range(d_all.shape[1] // HEAD_DIM):
        cols = slice(g * HEAD_DIM, (g + 1) * HEAD_DIM)
        prod = (d_all[:, cols].astype(F32) * o_ref[:, cols].astype(F32)).T
        total = all8(jnp.sum(prod, axis=0, keepdims=True))
        for i in range(total.shape[1] // chunk):
            dl_ref[i // 2, i % 2, :, cols] = total[:, i * chunk:(i + 1) * chunk]


def d_attn_of(dy, w_o, o_h, h, tile=512):
    n_all, d_model = dy.shape
    width = o_h.shape[1]
    rows = tile // (2 * HEAD_DIM)
    return pl.pallas_call(
        d_attn_kernel,
        grid=(n_all // tile,),
        in_specs=[
            pl.BlockSpec((tile, d_model), lambda i: (i, 0)),
            pl.BlockSpec((width, d_model), lambda i: (h, 0)),
            pl.BlockSpec((tile, width), lambda i: (i, 0)),
        ],
        out_specs=[
            pl.BlockSpec((tile, width), lambda i: (i, 0)),
            pl.BlockSpec((rows, 2, 8, width), lambda i: (i, 0, 0, 0)),
        ],
        out_shape=[
            jax.ShapeDtypeStruct((n_all, width), BF16),
            jax.ShapeDtypeStruct((n_all // (2 * HEAD_DIM), 2, 8, width), F32),
        ],
        compiler_params=params(),
        cost_estimate=pl.CostEstimate(flops=2 * n_all * d_model * width, bytes_accessed=2 * n_all * d_model + 2 * d_model * width, transcendentals=0),
    )(dy, w_o, o_h)


def pair_list(group):
    return [(2 * j, min(2, group - 2 * j)) for j in range((group + 1) // 2)]


def block_place(b, n_dev):
    half = (b >= n_dev // 2).astype(jnp.int32)
    dev = 2 * jnp.where(half == 1, n_dev - 1 - b, b)
    return dev, half


def block_mask(b, half, lo_row, hi_row):
    key = rows8(lax.broadcasted_iota(jnp.int32, (2 * HEAD_DIM, HEAD_DIM), 0))
    key = (key ^ (half * HEAD_DIM)) + b * (2 * HEAD_DIM)
    return (key >= lo_row) & (key <= hi_row)


def block_list(c, row, lo_sm, full_sm, qc_sm):
    lo, full, last = lo_sm[row, c], full_sm[row, c], qc_sm[c] // 2
    n_plain = last - full
    n_all = n_plain + full - lo + 1

    def block(t):
        m = lo + t - n_plain
        return jnp.where(t < n_plain, full + t, jnp.where(m < full, m, last))

    return n_plain, n_all, block


def run_blocks(blocks, first, step, even, odd):
    n_plain, n_all, block = blocks
    first(block(0))

    def pair(use_mask):
        def one(i, carry):
            t = 2 * i
            step(even, odd, block(t), block(t + 1), use_mask)
            step(odd, even, block(t + 1), block(t + 2), use_mask)
            return carry

        return one

    lax.fori_loop(0, n_plain // 2, pair(False), 0)
    lax.fori_loop(n_plain // 2, n_all // 2, pair(True), 0)

    @pl.when(n_all % 2 == 1)
    def _():
        step(even, None, block(n_all - 1), None, True)


def attn_fwd_kernel(lo_sm, full_sm, qc_sm, q_ref, kv_ref, lim_ref, o_ref, ot_ref, lse_ref, vt, qs, m_ref, l_ref, acc, s_a, s_b, *, group):
    row = pl.program_id(0)
    n_dev = kv_ref.shape[0]
    chunk = HEAD_DIM

    def key_block(b):
        dev, half = block_place(b, n_dev)
        return kv_ref.at[pl.ds(dev, 2), 0, half, 0]

    def turn(b, carry):
        v = key_block(b)[:, :, HEAD_DIM:].reshape(2 * chunk, HEAD_DIM)
        vt[b] = v.T
        return carry

    lax.fori_loop(jnp.minimum(lo_sm[row, 0], lo_sm[row, 1]), qc_sm[1] // 2 + 1, turn, 0)
    spans = [(slice(g0 * chunk, (g0 + ng) * chunk), ng) for g0, ng in pair_list(group)]
    n_span = len(spans)

    def one_chunk(c, carry):
        base = pl.multiple_of(c * chunk, chunk)
        for g in range(group):
            qs[g * chunk:(g + 1) * chunk, :] = q_ref[pl.ds(base, chunk), g * HEAD_DIM:(g + 1) * HEAD_DIM]
        m_ref[...] = jnp.full_like(m_ref, NEG_BIG)
        l_ref[...] = jnp.zeros_like(l_ref)
        acc[...] = jnp.zeros_like(acc)
        lo_row, hi_row = lim_ref[0, c, 0], lim_ref[0, c, 1]

        def keys_of(b):
            return key_block(b)[:, :, :HEAD_DIM].reshape(2 * chunk, HEAD_DIM)

        def step(now, later, b, b_next, use_mask):
            v_t = vt[b]

            def score(j):
                if later is not None and j < n_span:
                    cols = spans[j][0]
                    later[:, cols] = dotf(keys_of(b_next), qs[cols, :], NT)

            if use_mask:
                _, half = block_place(b, n_dev)
                ok = block_mask(b, half, lo_row, hi_row)
            score(0)
            for j, (cols, ng) in enumerate(spans):
                score(j + 1)
                s = rows8(now[:, cols])
                if use_mask:
                    s = jnp.concatenate([jnp.where(ok, s[:, :, i * chunk:(i + 1) * chunk], NEG_BIG) for i in range(ng)], axis=2)
                m_old = m_ref[:, cols]
                m_new = jnp.maximum(m_old, all8(jnp.max(jnp.max(s, axis=0), axis=0, keepdims=True)))
                p = jnp.exp2((s - m_new) * SCALE2)
                alpha = jnp.exp2((m_old - m_new) * SCALE2)
                m_ref[:, cols] = m_new
                l_ref[:, cols] = l_ref[:, cols] * alpha + jnp.sum(p, axis=0)
                acc[:, cols] = rows8(rows8(acc[:, cols]) * alpha) + dotf(v_t, rows8(p).astype(BF16), NN)

        def first(b):
            k = keys_of(b)
            for cols, _ in spans:
                s_a[:, cols] = dotf(k, qs[cols, :], NT)

        run_blocks(block_list(c, row, lo_sm, full_sm, qc_sm), first, step, s_a, s_b)
        l_all = all8(jnp.sum(l_ref[...], axis=0, keepdims=True))
        inv_l = 1.0 / l_all
        lse_ref[0, c] = m_ref[...] * SCALE2 + jnp.log(l_all) * LOG2E
        for g in range(group):
            cols = slice(g * chunk, (g + 1) * chunk)
            o_t = rows8(rows8(acc[:, cols]) * inv_l[:, cols])
            o_ref[pl.ds(base, chunk), cols] = o_t.T.astype(BF16)
            ot_ref[cols, pl.ds(base, chunk)] = o_t.astype(BF16)
        return carry

    lax.fori_loop(0, 2, one_chunk, 0)


def attn_cost(n_rows, n_dev, width, n_mat):
    pairs = n_rows * (2 * n_dev + 1) * 128 * 128 * (width // HEAD_DIM)
    return pl.CostEstimate(flops=4 * n_mat * pairs * HEAD_DIM, bytes_accessed=8 * n_rows * 256 * width, transcendentals=pairs)


def attn_fwd(scalars, q, kv, at, limits):
    n_all, width = q.shape
    n_dev, _, _, n_rows, chunk, _ = kv.shape
    group = width // HEAD_DIM
    n_tok = n_all // n_rows
    return pl.pallas_call(
        functools.partial(attn_fwd_kernel, group=group),
        grid_spec=pltpu.PrefetchScalarGridSpec(
            num_scalar_prefetch=3,
            grid=(n_rows,),
            in_specs=[
                pl.BlockSpec((n_tok, width), lambda i, *_: (i, 0)),
                pl.BlockSpec((n_dev, 1, 2, 1, chunk, 2 * HEAD_DIM), lambda i, *_: (0, at, 0, i, 0, 0)),
                pl.BlockSpec((1, 2, 2, 8, chunk), lambda i, *_: (i, 0, 0, 0, 0)),
            ],
            out_specs=[
                pl.BlockSpec((n_tok, width), lambda i, *_: (i, 0)),
                pl.BlockSpec((width, n_tok), lambda i, *_: (0, i)),
                pl.BlockSpec((1, 2, 8, width), lambda i, *_: (i, 0, 0, 0)),
            ],
            scratch_shapes=[
                pltpu.VMEM((n_dev, HEAD_DIM, 2 * chunk), BF16),
                pltpu.VMEM((group * chunk, HEAD_DIM), BF16),
                pltpu.VMEM((8, width), F32),
                pltpu.VMEM((8, width), F32),
                pltpu.VMEM((HEAD_DIM, width), F32),
                pltpu.VMEM((2 * chunk, width), F32),
                pltpu.VMEM((2 * chunk, width), F32),
            ],
        ),
        out_shape=[
            jax.ShapeDtypeStruct((n_all, width), BF16),
            jax.ShapeDtypeStruct((width, n_all), BF16),
            jax.ShapeDtypeStruct((n_rows, 2, 8, width), F32),
        ],
        compiler_params=params(),
        cost_estimate=attn_cost(n_rows, n_dev, width, 2),
    )(*scalars, q, kv, limits)


def attn_bwd_kernel(lo_sm, full_sm, qc_sm, q_ref, kv_ref, lim_ref, do_ref, lse_ref, dl_ref, cos_ref, sin_ref, dq_ref, keep_ref, send_ref, kt, qs, dos, dqt, dkv_ref, s_a, s_b, d_a, d_b, *, group):
    row = pl.program_id(0)
    n_dev = kv_ref.shape[0]
    chunk = HEAD_DIM
    dkv_ref[...] = jnp.zeros_like(dkv_ref)

    def key_block(b):
        dev, half = block_place(b, n_dev)
        return kv_ref.at[pl.ds(dev, 2), 0, half, 0]

    def turn(b, carry):
        k = key_block(b)[:, :, :HEAD_DIM].reshape(2 * chunk, HEAD_DIM)
        kt[b] = k.T
        return carry

    lax.fori_loop(jnp.minimum(lo_sm[row, 0], lo_sm[row, 1]), qc_sm[1] // 2 + 1, turn, 0)
    spans = [(slice(g0 * chunk, (g0 + ng) * chunk), ng) for g0, ng in pair_list(group)]

    def one_chunk(c, carry):
        base = pl.multiple_of(c * chunk, chunk)
        for g in range(group):
            cols = slice(g * HEAD_DIM, (g + 1) * HEAD_DIM)
            qs[g * chunk:(g + 1) * chunk, :] = q_ref[pl.ds(base, chunk), cols]
            dos[g * chunk:(g + 1) * chunk, :] = do_ref[pl.ds(base, chunk), cols]
        dqt[...] = jnp.zeros_like(dqt)
        lo_row, hi_row = lim_ref[0, c, 0], lim_ref[0, c, 1]

        def keys_of(b):
            kv = key_block(b)[...].reshape(2 * chunk, 2 * HEAD_DIM)
            return kv[:, :HEAD_DIM], kv[:, HEAD_DIM:]

        def score(later, k, v, j):
            cols = spans[j][0]
            later[0][:, cols] = dotf(k, qs[cols, :], NT)
            later[1][:, cols] = dotf(v, dos[cols, :], NT)

        def step(now, later, b, b_next, use_mask):
            dev, half = block_place(b, n_dev)
            k_t = kt[b]
            if use_mask:
                ok = block_mask(b, half, lo_row, hi_row)
            dk = jnp.zeros((2 * chunk, HEAD_DIM), F32)
            dv = jnp.zeros((2 * chunk, HEAD_DIM), F32)

            def ahead(j):
                if later is not None and j < len(spans):
                    score(later, *keys_of(b_next), j)

            ahead(0)
            for j, (cols, ng) in enumerate(spans):
                ahead(j + 1)
                p = jnp.exp2(rows8(now[0][:, cols]) * SCALE2 - lse_ref[0, c, :, cols])
                if use_mask:
                    p = jnp.concatenate([jnp.where(ok, p[:, :, i * chunk:(i + 1) * chunk], 0.0) for i in range(ng)], axis=2)
                ds = rows8(p * (rows8(now[1][:, cols]) - dl_ref[0, c, :, cols])).astype(BF16)
                dv = dv + dotf(rows8(p).astype(BF16), dos[cols, :], NN)
                dk = dk + dotf(ds, qs[cols, :], NN)
                dqt[:, cols] += dotf(k_t, ds, NN)
            out = dkv_ref.at[pl.ds(dev, 2), half]
            out[:, :, :HEAD_DIM] += (dk * SCALE).reshape(2, chunk, HEAD_DIM)
            out[:, :, HEAD_DIM:] += dv.reshape(2, chunk, HEAD_DIM)

        def first(b):
            for j in range(len(spans)):
                score((s_a, d_a), *keys_of(b), j)

        run_blocks(block_list(c, row, lo_sm, full_sm, qc_sm), first, step, (s_a, d_a), (s_b, d_b))
        cos_t, sin_t = cos_ref[0, c], sin_ref[0, c]
        for g in range(group):
            cols = slice(g * chunk, (g + 1) * chunk)
            d = dqt[:, cols] * SCALE
            a, b = d[:HEAD_DIM // 2], d[HEAD_DIM // 2:]
            turned = jnp.concatenate([a * cos_t + b * sin_t, b * cos_t - a * sin_t], axis=0)
            dq_ref[pl.ds(base, chunk), cols] = turned.T.astype(BF16)
        return carry

    lax.fori_loop(0, 2, one_chunk, 0)
    core = qc_sm[2]
    for i in range(n_dev // 2):
        for half in range(2):
            keep_ref[i, half, 0] = dkv_ref[2 * i + core, half]
            send_ref[i, half, 0] = dkv_ref[2 * i + 1 - core, half]


def attn_bwd(scalars, q, kv, at, limits, d_o, lse, delta, cos_c, sin_c):
    n_all, width = q.shape
    n_dev, _, _, n_rows, chunk, _ = kv.shape
    group = width // HEAD_DIM
    n_tok = n_all // n_rows
    tok = pl.BlockSpec((n_tok, width), lambda i, *_: (i, 0))
    kvs = pl.BlockSpec((n_dev, 1, 2, 1, chunk, 2 * HEAD_DIM), lambda i, *_: (0, at, 0, i, 0, 0))
    dkvs = pl.BlockSpec((n_dev // 2, 2, 1, chunk, 2 * HEAD_DIM), lambda i, *_: (0, 0, i, 0, 0))
    stat = pl.BlockSpec((1, 2, 8, width), lambda i, *_: (i, 0, 0, 0))
    rope = pl.BlockSpec((1, 2, HEAD_DIM // 2, chunk), lambda i, *_: (i, 0, 0, 0))
    return pl.pallas_call(
        functools.partial(attn_bwd_kernel, group=group),
        grid_spec=pltpu.PrefetchScalarGridSpec(
            num_scalar_prefetch=3,
            grid=(n_rows,),
            in_specs=[tok, kvs, pl.BlockSpec((1, 2, 2, 8, chunk), lambda i, *_: (i, 0, 0, 0, 0)), tok, stat, stat, rope, rope],
            out_specs=[tok, dkvs, dkvs],
            scratch_shapes=[
                pltpu.VMEM((n_dev, HEAD_DIM, 2 * chunk), BF16),
                pltpu.VMEM((group * chunk, HEAD_DIM), BF16),
                pltpu.VMEM((group * chunk, HEAD_DIM), BF16),
                pltpu.VMEM((HEAD_DIM, width), F32),
                pltpu.VMEM((n_dev, 2, chunk, 2 * HEAD_DIM), F32),
            ] + [pltpu.VMEM((2 * chunk, width), F32)] * 4,
        ),
        out_shape=[jax.ShapeDtypeStruct((n_all, width), BF16)]
        + [jax.ShapeDtypeStruct((n_dev // 2, 2, n_rows, chunk, 2 * HEAD_DIM), F32)] * 2,
        compiler_params=params(),
        cost_estimate=attn_cost(n_rows, n_dev, width, 5),
    )(*scalars, q, kv, limits, d_o, lse, delta, cos_c, sin_c)


def grid_spec(n_prefetch, grid, in_specs, out_specs):
    return pltpu.PrefetchScalarGridSpec(num_scalar_prefetch=n_prefetch, grid=grid, in_specs=in_specs, out_specs=out_specs)


def both_tokens(own_ref, pair_ref, rhs_ref, rhs_pair_ref):
    return dotf(own_ref[...], rhs_ref[...], NN) + dotf(pair_ref[...], rhs_pair_ref[...], NN)


def grad_parts_kernel(order_sm, own_ref, pair_ref, rhs_ref, rhs_pair_ref, sx_ref, sy_ref, k_ref):
    i = pl.program_id(0)
    part = both_tokens(own_ref, pair_ref, rhs_ref, rhs_pair_ref)

    @pl.when(i < 2)
    def _():
        sx_ref[0] = part

    @pl.when((i >= 2) & (i < 4))
    def _():
        sy_ref[0] = part

    @pl.when(i >= 4)
    def _():
        k_ref[0] = part


def grad_specs(rhs, tile, own_at, pair_at):
    n_all, cols = rhs.shape
    whole = pl.BlockSpec((n_all, cols), lambda i, *_: (0, 0), pipeline_mode=pl.Buffered(1))
    cost = pl.CostEstimate(flops=4 * 8 * tile * n_all * cols, bytes_accessed=4 * n_all * (8 * tile + cols) + 32 * tile * cols, transcendentals=0)
    return [pl.BlockSpec((tile, n_all), own_at), pl.BlockSpec((tile, n_all), pair_at), whole, whole], cost


def grad_parts(order, own, pair, rhs, rhs_pair):
    tile, cols = pair.shape[0] // 8, rhs.shape[1]
    own_base = lambda order: order[8] if own.shape[0] > pair.shape[0] else 0
    in_specs, cost = grad_specs(rhs, tile, lambda i, order: (order[i] + own_base(order), 0), lambda i, order: (order[i], 0))
    block = (1, tile, cols)
    return pl.pallas_call(
        grad_parts_kernel,
        grid_spec=grid_spec(1, (8,), in_specs, [
            pl.BlockSpec(block, lambda i, order: (jnp.minimum(i, 1), 0, 0)),
            pl.BlockSpec(block, lambda i, order: (jnp.clip(i - 2, 0, 1), 0, 0)),
            pl.BlockSpec(block, lambda i, order: (jnp.maximum(i - 4, 0), 0, 0))]),
        out_shape=[jax.ShapeDtypeStruct((n, tile, cols), F32) for n in (2, 2, 4)],
        compiler_params=params(),
        cost_estimate=cost,
    )(order, own, pair, rhs, rhs_pair)


def grad_whole_kernel(order_sm, own_ref, pair_ref, rhs_ref, rhs_pair_ref, o_ref):
    o_ref[...] = both_tokens(own_ref, pair_ref, rhs_ref, rhs_pair_ref)


def grad_whole(order, own, pair, rhs, rhs_pair):
    tile, cols = pair.shape[0] // 8, rhs.shape[1]
    in_specs, cost = grad_specs(rhs, tile, lambda i, order: (i + order[8], 0), lambda i, order: (i, 0))
    return pl.pallas_call(
        grad_whole_kernel,
        grid_spec=grid_spec(1, (8,), in_specs, [pl.BlockSpec((tile, cols), lambda i, order: (i, 0))]),
        out_shape=[jax.ShapeDtypeStruct((8 * tile, cols), F32)],
        compiler_params=params(),
        cost_estimate=cost,
    )(order, own, pair, rhs, rhs_pair)[0]


def add_parts_kernel(at_sm, a_ref, b_ref, c_ref, d_ref, ra_ref, rb_ref, rc_ref, rd_ref, *o_refs):
    for o_ref, k_ref, r_ref in zip(o_refs, (a_ref, b_ref, c_ref, d_ref), (ra_ref, rb_ref, rc_ref, rd_ref)):
        o_ref[...] = k_ref[0] + r_ref[0]


def add_parts(at, kept, rx, ry):
    _, rows, cols = kept.shape
    n = 2
    block = (1, rows // n, cols)
    part = lambda j: pl.BlockSpec(block, lambda i, at: (j, i, 0))
    recv = lambda f: pl.BlockSpec(block, lambda i, at: (f(at[0], at[1]), i, 0))
    out = pl.BlockSpec((rows // n, cols), lambda i, at: (i, 0))
    return pl.pallas_call(
        add_parts_kernel,
        grid_spec=grid_spec(1, (n,), [part(j) for j in range(4)] + [
            recv(lambda x, y: y), recv(lambda x, y: 1 - y), recv(lambda x, y: x), recv(lambda x, y: 1 - x)], [out] * 4),
        out_shape=[jax.ShapeDtypeStruct((rows, cols), F32)] * 4,
        compiler_params=params(),
        cost_estimate=pl.CostEstimate(flops=2 * kept.size, bytes_accessed=12 * kept.size, transcendentals=0),
        name="add_parts",
    )(at, *([kept] * 4), rx, rx, ry, ry)


def add_last_kernel(a_ref, ra_ref, b_ref, rb_ref, o_ref):
    o_ref[0] = a_ref[...] + ra_ref[...]
    o_ref[1] = b_ref[...] + rb_ref[...]


def add_last(k1, r1, k2, r2):
    rows, cols = k1.shape
    n = 2
    one = pl.BlockSpec((rows // n, cols), lambda i: (i, 0))
    return pl.pallas_call(
        add_last_kernel,
        grid=(n,),
        in_specs=[one] * 4,
        out_specs=pl.BlockSpec((2, rows // n, cols), lambda i: (0, i, 0)),
        out_shape=jax.ShapeDtypeStruct((2, rows, cols), F32),
        compiler_params=params(),
        cost_estimate=pl.CostEstimate(flops=2 * k1.size, bytes_accessed=24 * k1.size, transcendentals=0),
        name="add_last",
    )(k1, r1, k2, r2)


def sum_core_kernel(at_sm, keep_ref, got_ref, kx_ref, sx_ref, ky_ref, sy_ref):
    x, y = at_sm[0], at_sm[1]
    for i in range(2):
        for o_ref, j in ((kx_ref, x), (sx_ref, 1 - x)):
            o_ref[i, 0] = keep_ref[i, j, 0, 0] + got_ref[i, j, 0, 0]
        for o_ref, j in ((ky_ref, y), (sy_ref, 1 - y)):
            o_ref[i, 0] = keep_ref[j, i, 1, 0] + got_ref[j, i, 1, 0]


def sum_core(at, keep, got):
    shape = keep.shape[3:]
    cells = pl.BlockSpec((2, 2, 2, 1) + shape[1:], lambda i, *_: (0, 0, 0, i, 0, 0))
    pair = pl.BlockSpec((2, 1) + shape[1:], lambda i, *_: (0, i, 0, 0))
    return pl.pallas_call(
        sum_core_kernel,
        grid_spec=pltpu.PrefetchScalarGridSpec(num_scalar_prefetch=1, grid=(shape[0],), in_specs=[cells] * 2, out_specs=[pair] * 4),
        out_shape=[jax.ShapeDtypeStruct((2,) + shape, F32)] * 4,
        compiler_params=params(),
        cost_estimate=pl.CostEstimate(flops=8 * keep.size, bytes_accessed=12 * keep.size, transcendentals=0),
        name="sum_core",
    )(at, keep, got)


def sum_axis_kernel(at_sm, kx_ref, rx_ref, ky_ref, ry_ref, k1_ref, s1_ref, k2_ref, s2_ref):
    x, y = at_sm[0], at_sm[1]
    for o_ref, j in ((k1_ref, y), (s1_ref, 1 - y)):
        o_ref[0] = kx_ref[j, 0] + rx_ref[j, 0]
    for o_ref, j in ((k2_ref, x), (s2_ref, 1 - x)):
        o_ref[0] = ky_ref[j, 0] + ry_ref[j, 0]


def sum_axis(at, kx, rx, ky, ry):
    shape = kx.shape[1:]
    pair = pl.BlockSpec((2, 1) + shape[1:], lambda i, *_: (0, i, 0, 0))
    one = pl.BlockSpec((1,) + shape[1:], lambda i, *_: (i, 0, 0))
    return pl.pallas_call(
        sum_axis_kernel,
        grid_spec=pltpu.PrefetchScalarGridSpec(num_scalar_prefetch=1, grid=(shape[0],), in_specs=[pair] * 4, out_specs=[one] * 4),
        out_shape=[jax.ShapeDtypeStruct(shape, F32)] * 4,
        compiler_params=params(),
        cost_estimate=pl.CostEstimate(flops=8 * kx.size, bytes_accessed=24 * kx.size, transcendentals=0),
        name="sum_axis",
    )(at, kx, rx, ky, ry)


def sum_last_kernel(cos_ref, sin_ref, *refs):
    *in_refs, o_ref = refs
    chunk = HEAD_DIM
    for h in range(len(in_refs) // 4):
        for half in range(2):
            a_ref, b_ref = in_refs[4 * h + 2 * half], in_refs[4 * h + 2 * half + 1]
            rows = slice(half * chunk, (half + 1) * chunk)
            total = a_ref[0] + b_ref[0]
            dk = total[:, :HEAD_DIM]
            dk = dk * cos_ref[0, rows] - pltpu.roll(dk, HEAD_DIM // 2, 1) * sin_ref[0, rows]
            at_k, at_v = h * HEAD_DIM, o_ref.shape[1] // 2 + h * HEAD_DIM
            o_ref[rows, at_k:at_k + HEAD_DIM] = dk.astype(BF16)
            o_ref[rows, at_v:at_v + HEAD_DIM] = total[:, HEAD_DIM:].astype(BF16)


def sum_last(cos_t, sin_t, parts):
    n_rows, n_tok, _ = cos_t.shape
    shape = parts[0].shape
    rope = pl.BlockSpec((1, n_tok, HEAD_DIM), lambda i: (i, 0, 0))
    one = pl.BlockSpec((1,) + shape[1:], lambda i: (i, 0, 0))
    cols = len(parts) // 4 * shape[2]
    return pl.pallas_call(
        sum_last_kernel,
        grid=(n_rows,),
        in_specs=[rope] * 2 + [one] * len(parts),
        out_specs=pl.BlockSpec((n_tok, cols), lambda i: (i, 0)),
        out_shape=jax.ShapeDtypeStruct((n_rows * n_tok, cols), BF16),
        compiler_params=params(),
        cost_estimate=pl.CostEstimate(flops=8 * parts[0].size * len(parts), bytes_accessed=4 * parts[0].size * len(parts), transcendentals=0),
        name="sum_last",
    )(cos_t, sin_t, *parts)


def copy_kernel(i_ref, *refs):
    o_ref = refs[-1]
    o_ref[...] = i_ref[...].reshape(o_ref.shape)


def split_kernel(i_ref, k_ref, v_ref):
    k_ref[...] = i_ref[0, :, :k_ref.shape[1]]
    v_ref[...] = i_ref[0, :, k_ref.shape[1]:]


def place(x, grid, in_spec, outs, kernel=copy_kernel, into=None):
    return pl.pallas_call(
        kernel,
        grid=grid,
        in_specs=[in_spec] + [pl.BlockSpec(memory_space=pl.ANY)] * (into is not None),
        out_specs=[spec for _, spec in outs],
        out_shape=[jax.ShapeDtypeStruct(shape, x.dtype) for shape, _ in outs],
        input_output_aliases={} if into is None else {1: 0},
        compiler_params=params(),
        cost_estimate=pl.CostEstimate(flops=x.size, bytes_accessed=8 * x.size, transcendentals=0),
    )(*([x] if into is None else [x, into]))


def solution(mesh):
    n_dev = mesh.shape['cp']

    def block(hidden, grad_out, positions, seg_ids, w_q, w_k, w_v, w_o, norm_gain):
        n_batch, n_tok, d_model = hidden.shape
        n_all = n_batch * n_tok
        chunk = n_tok // 2
        kv_heads = w_k.shape[1] // HEAD_DIM
        width = w_q.shape[1] // kv_heads
        heads = range(kv_heads)
        rank = lax.axis_index('cp')

        q_chunks = jnp.stack([rank, 2 * n_dev - 1 - rank, rank & 1]).astype(jnp.int32)
        glob = (q_chunks[:2, None] * chunk + jnp.arange(chunk, dtype=jnp.int32)[None, :])
        pos_c = positions.reshape(n_batch, 2, chunk)
        doc_start = glob[None] - pos_c
        limits = jnp.stack([doc_start, jnp.broadcast_to(glob[None], doc_start.shape)], axis=2)
        limits = jnp.broadcast_to(limits[:, :, :, None], (n_batch, 2, 2, 8, chunk))
        blk = 2 * chunk
        last = q_chunks[:2] // 2
        lo_blk = doc_start[:, :, 0] // blk
        full_blk = jnp.minimum((doc_start[:, :, -1] + blk - 1) // blk, last[None, :])
        scalars = (lo_blk, full_blk, q_chunks)

        inv_freq = ROPE_BASE ** (-jnp.arange(0, HEAD_DIM, 2).astype(F32) / HEAD_DIM)
        pos_f = positions.astype(F32)
        ang = pos_f[..., None] * inv_freq
        cos_h, sin_h = jnp.cos(ang), jnp.sin(ang)
        cos_t = jnp.concatenate([cos_h, cos_h], axis=-1)
        sin_t = jnp.concatenate([-sin_h, sin_h], axis=-1)
        cos_c = jnp.swapaxes(cos_h.reshape(n_batch, 2, chunk, HEAD_DIM // 2), 2, 3)
        sin_c = jnp.swapaxes(sin_h.reshape(n_batch, 2, chunk, HEAD_DIM // 2), 2, 3)

        cos_t, sin_t = lax.optimization_barrier((cos_t, sin_t))
        core, at = rank & 1, jnp.stack([(rank >> 1) & 1, (rank >> 2) & 1]).astype(jnp.int32)

        def send(value, bit):
            return lax.ppermute(value, 'cp', [(i, i ^ bit) for i in range(n_dev)])

        x_at, y_at = at[0], at[1]
        cell = lambda y, x, half: (y * 2 + x) * 2 + half
        order = jnp.stack(
            [cell(0, 1 - x_at, 0), cell(1, 1 - x_at, 0), cell(1 - y_at, 0, 1), cell(1 - y_at, 1, 1)]
            + [cell(y_at, x_at, 0), cell(1 - y_at, x_at, 0), cell(y_at, x_at, 1), cell(y_at, 1 - x_at, 1), 8 * core]).astype(jnp.int32)

        def share(own, pair, rhs, rhs_pair):
            sx, sy, kept = grad_parts(order, own, pair, rhs, rhs_pair)
            rx, ry = send(sx, 2), send(sy, 4)
            k1, s1, k2, s2 = add_parts(at, kept, rx, ry)
            r1, r2 = send(s1, 4), send(s2, 2)
            total = add_last(k1, r1, k2, r2)
            return total.reshape(-1, total.shape[-1])

        def half_cols(value, which):
            return lax.dynamic_slice_in_dim(value, which * (d_model // 2), d_model // 2, 1)

        same_core = [[i + j for i in range(0, n_dev, 2)] for j in range(2)]
        scatter = functools.partial(lax.psum_scatter, axis_name='cp', scatter_dimension=0, axis_index_groups=same_core, tiled=True)
        gather = functools.partial(lax.all_gather, axis_name='cp', axis=0, tiled=False)

        normed, *kv_loc = norm_kv(hidden, norm_gain, w_k, w_v, cos_t, sin_t)
        kv_parts = []
        for part in kv_loc:
            kv_parts.append(gather(part))
        kv_of = [(kv_parts[0], 0)] + [(kv_parts[-1], h - 1) for h in heads[1:]]

        dy = grad_out.reshape(n_all, d_model)
        dy_own, dy_pair = half_cols(dy, core), send(half_cols(dy, 1 - core), 1)
        n_t = turned(normed)
        n_pair = send(lax.dynamic_slice_in_dim(n_t, (1 - core) * (d_model // 2), d_model // 2, 0), 1)
        q, attn, gwo, dq, dkv, gwq = [], [], [], [], [], []
        for h in heads:
            q.append(q_proj(normed, w_q, cos_t, sin_t, h, width))
            o_h, ot_h, lse_h = attn_fwd(scalars, q[h], *kv_of[h], limits)
            attn.append(o_h)
            own = share(ot_h, send(ot_h, 1), dy_own, dy_pair)
            gwo.append(gather(own))
            d_attn_h, delta_h = d_attn_of(dy, w_o, o_h, h)
            dq_h, keep, give = attn_bwd(scalars, q[h], *kv_of[h], limits, d_attn_h, lse_h, delta_h, cos_c, sin_c)
            dq.append(dq_h)
            own = share(n_t, n_pair, dq_h, send(dq_h, 1))
            gwq.append(gather(own))
            got = send(give, 1)
            cells = (2, 2) + keep.shape[1:]
            kx, sx, ky, sy = sum_core(at, keep.reshape(cells), got.reshape(cells))
            rx, ry = send(sx, 2), send(sy, 4)
            k1, s1, k2, s2 = sum_axis(at, kx, rx, ky, ry)
            dkv += [k1, send(s1, 4), k2, send(s2, 2)]

        attn_flat = jnp.concatenate(attn, axis=1)
        proj_out = dotf(attn_flat, w_o, NN).reshape(hidden.shape)
        block_out = (hidden.astype(F32) + proj_out).astype(BF16)
        dq_flat = jnp.concatenate(dq, axis=1)
        d_norm_q = dotf(dq_flat, w_q, NT)

        dkv_lin = sum_last(cos_t, sin_t, dkv)
        dkv_pair = send(dkv_lin, 1)
        part = grad_whole(order, n_t, n_pair, dkv_lin, dkv_pair)
        gwkv = scatter(part)

        w_kv = jnp.concatenate([w_k, w_v], axis=1)
        d_norm_kv = dotf(dkv_lin, w_kv, NT)
        d_normed = (d_norm_q + d_norm_kv).astype(BF16).astype(F32)
        x = hidden.astype(F32).reshape(n_all, d_model)
        inv = lax.rsqrt(jnp.mean(x * x, axis=-1, keepdims=True) + NORM_EPS)
        xn = x * inv
        u = d_normed * norm_gain.astype(F32)
        d_x = inv * (u - xn * jnp.mean(u * xn, axis=-1, keepdims=True))
        grad_hidden = (dy.astype(F32) + d_x).astype(BF16).reshape(hidden.shape)
        grad_gain = jnp.sum(d_normed * xn, axis=0)
        for bit in (1, 2, 4):
            grad_gain = grad_gain + send(grad_gain, bit)
        gwkv_all = gather(gwkv)

        n_chip = n_dev // 2
        rows_o, rows_q = width // n_chip, d_model // n_dev
        grad_wo = grad_wq = None
        for h in heads:
            grad_wo, = place(
                gwo[h], (n_dev,), pl.BlockSpec((1, rows_o, d_model // 2), lambda d: (d, 0, 0)),
                [(w_o.shape, pl.BlockSpec((rows_o, d_model // 2), lambda d, h=h: (h * n_chip + d // 2, d % 2)))], into=grad_wo)
        at_q = lambda d: ((d % 2) * n_chip + d // 2, 0)
        for h in heads:
            grad_wq, = place(
                gwq[h], (n_dev,), pl.BlockSpec((1, rows_q, width), lambda d: (d, 0, 0)),
                [(w_q.shape, pl.BlockSpec((rows_q, width), lambda d, h=h: (at_q(d)[0], h)))], into=grad_wq)
        grad_wk, grad_wv = place(
            gwkv_all, (n_dev,), pl.BlockSpec((1, rows_q, 2 * w_k.shape[1]), lambda d: (d, 0, 0)),
            [(w_k.shape, pl.BlockSpec((rows_q, w_k.shape[1]), at_q))] * 2, split_kernel)
        return block_out, grad_hidden, grad_wq, grad_wk, grad_wv, grad_wo, grad_gain

    seq_spec = P(None, 'cp', None)
    tok_spec = P(None, 'cp')
    full = P()
    return jax.shard_map(block, mesh=mesh, in_specs=(seq_spec, seq_spec, tok_spec, tok_spec, full, full, full, full, full), out_specs=(seq_spec, seq_spec, full, full, full, full, full), check_vma=False)
```
